32 devices in a mesh: groups: 2 (over x), col: 16 (over z, y, core).
Axes of the slice: x: 2, y: 2, z: 4, core: 2. Of those that a mesh axis runs over, the one named last changes fastest.
Arguments:
- left: bfloat16 [256, 64, 32], P('col', 'groups'), parts along dimension 1, may hold values from -18 to 18
- right: bfloat16 [256, 2560, 32], P('col', 'groups'), parts along dimension 1, may hold values from -18 to 18
- out_weight: bfloat16 [1024, 128], replicated, may hold values from -0.1875 to 0.1875
- out_bias: float32 [128], replicated, may hold values from -3 to 3
Outputs:
- pair_update: bfloat16 [64, 1280, 128], P('groups', 'col'), parts along dimension 0
The draws below stay inside these ranges and needn't reach their ends.
There are 2 independent parts, one for each index of `groups`. The reference program is written for one: setup_inputs(seed, part) draws one part's arguments, and reference() takes and returns one part's arrays. A program takes and returns all parts, laid end to end along the dimension named above; an argument that names none is the same for every part. Nothing has to cross between parts.
All inputs are finite; a program needn't handle non-finite values.
Results may differ from the reference program's by a relative error of at most 0.004.
Values may be sent and summed in bfloat16 or wider, within the bound.
A program may use at most 64 MiB of HBM per device.

```python
import jax
import jax.numpy as jnp
from jax import lax

C = 32
PAIR = 128
S = 256
COL_DEV = 80
R = 1280
ROWS = 32
CC = 1024
N_COL = 16


def levels(own_key, dims, split, low, largest):
    def one(dim, shards_of):
        heights = jax.random.uniform(jax.random.fold_in(jax.random.fold_in(own_key, 6), dim), (shards_of,), jnp.float32, low / len(split), largest / len(split))
        return jnp.repeat(jnp.exp(heights), dims[dim] // shards_of).reshape((-1,) + (1,) * (len(dims) - dim - 1))

    loudness = one(*split[0])
    for cut in split[1:]:
        loudness = loudness * one(*cut)
    return loudness


def bell_draw(rng, shape, deviation, limit, split=(), kind=jnp.bfloat16):
    level = levels(rng, shape, split, -0.22, 0.18) if split else 1.0
    result = jax.random.normal(rng, shape, jnp.float32) * deviation * level
    return jnp.minimum(jnp.maximum(result, -limit), limit).astype(kind)


def setup_inputs(seed: int = 0, part: int = 0) -> dict:
    key_list = jax.random.split(jax.random.key(seed), 5)
    part_keys = jax.random.split(jax.random.fold_in(key_list[4], part), 5)
    left = bell_draw(part_keys[0], (S, ROWS, C), 3.0, 18.0, ((0, 16),))
    right = bell_draw(part_keys[1], (S, R, C), 3.0, 18.0, ((0, 16),))
    out_weight = bell_draw(key_list[2], (CC, PAIR), CC ** -0.5, 0.1875)
    out_bias = bell_draw(key_list[3], (PAIR,), 0.5, 3.0, (), jnp.float32)
    return {"left": left, "right": right, "out_weight": out_weight, "out_bias": out_bias}


def reference(left, right, out_weight, out_bias):
    left_wide = left.astype(jnp.float32)
    right_wide = right.astype(jnp.float32)

    def column_block(index):
        start = (index * COL_DEV).astype(jnp.int32)
        block = lax.dynamic_slice_in_dim(right_wide, start, COL_DEV, 1)
        outer = jnp.einsum("sic,sje->ijce", left_wide, block, precision=lax.Precision.HIGHEST) / S
        flat = outer.astype(jnp.bfloat16).reshape(ROWS * COL_DEV, C * C)
        update = jnp.dot(flat, out_weight, preferred_element_type=jnp.float32) + out_bias
        return update.astype(jnp.bfloat16).reshape(ROWS, COL_DEV, PAIR)

    blocks = lax.map(column_block, jnp.arange(N_COL, dtype=jnp.int32))
    return jnp.transpose(blocks, (1, 0, 2, 3)).reshape(ROWS, N_COL * COL_DEV, PAIR)
```

```python
import functools
import math

import jax
import jax.numpy as jnp
from jax import lax
from jax.experimental import pallas as pl
from jax.experimental.pallas import tpu as pltpu
from jax.sharding import PartitionSpec as P

MESH = pl.DeviceIdType.MESH
LANES = 128
TILE = 16
GROUP = 4


def lane_index():
    return lax.broadcasted_iota(jnp.int32, (TILE, LANES), 1)


def turn_lanes(x, shift):
    shift %= LANES
    return pltpu.roll(x, shift, axis=1) if shift else x


def pick(lane, start, left, right):
    return jnp.where(lane >= start, right, left)


def pack_columns(cols, period, tiles):
    lane = lane_index()
    packed = []
    for d in range(period):
        first, offset = divmod(cols * d, LANES)
        moved = []
        for e in range(period):
            piece = tiles[e][first]
            if offset + cols > LANES:
                piece = pick(lane, offset, tiles[e][first + 1], piece)
            moved.append(turn_lanes(piece, cols * e - offset))
        outs = []
        for u in range(cols * period // LANES):
            low, high = u * LANES, (u + 1) * LANES
            out = None
            for e in range(period):
                start = cols * e
                if start + cols <= low or start >= high:
                    continue
                out = moved[e] if out is None else pick(lane, start - low, out, moved[e])
            outs.append(out)
        packed.append(outs)
    return packed


def unpack_columns(cols, period, tiles):
    lane = lane_index()
    wide = []
    for e in range(period):
        first, offset = divmod(cols * e, LANES)
        piece = tiles[first]
        if offset + cols > LANES:
            piece = pick(lane, offset, tiles[first + 1], piece)
        wide.append(turn_lanes(piece, -offset))
    return wide


def packed_kernel(
    n, cols, period, left_hbm, right_hbm, weight_hbm, bias_hbm, out_ref,
    left_ref, right_ref, weight_ref, bias_ref, lspread, rspread, sbuf, rbuf, lbuf,
    rwide, lturn, wturn, flat, partial,
    rsend, rrecv, lsend, lrecv, loads,
):
    me = lax.axis_index("col")
    half = n // 2
    base = me // half * half
    partner = me + 1 - 2 * lax.rem(me, 2)
    mirror = lax.rem(me + half, n)
    local, rows, width = left_ref.shape
    seqs = n * local
    chunks = width // period
    halves = width // TILE
    per_half = chunks // halves
    channels = width * width
    deep = period * width

    barrier = pltpu.get_barrier_semaphore()
    for k in range(1, n):
        pl.semaphore_signal(
            barrier, inc=1, device_id={"col": lax.rem(me + k, n)}, device_id_type=MESH
        )
    fetch_left = pltpu.make_async_copy(left_hbm, left_ref, loads.at[0])
    fetch_weight = pltpu.make_async_copy(weight_hbm, weight_ref, loads.at[1])
    fetch_bias = pltpu.make_async_copy(bias_hbm, bias_ref, loads.at[2])
    fetch_right = [
        pltpu.make_async_copy(
            right_hbm.at[:, pl.ds(h * TILE, TILE)],
            right_ref.at[:, pl.ds(h * TILE, TILE)],
            loads.at[3 + h],
        )
        for h in range(halves)
    ]
    fetch_left.start()
    for fetch in fetch_right:
        fetch.start()
    fetch_weight.start()
    fetch_bias.start()

    fetch_left.wait()
    for s in range(local):
        lspread[s * rows : (s + 1) * rows, :width] = left_ref[s].astype(jnp.float32)
    lane = lane_index()
    join = LANES // width
    for t in range(rows // join):
        block = lspread[pl.ds(t * join, local, stride=rows), :]
        for k in range(1, join):
            piece = lspread[pl.ds(t * join + k, local, stride=rows), :]
            block = pick(lane, k * width, block, turn_lanes(piece, k * width))
        lbuf[me, :, t * LANES : (t + 1) * LANES] = block.astype(jnp.bfloat16)

    turns = cols * period // LANES
    cycles = n // period
    for h in range(halves):
        fetch_right[h].wait()
        for s in range(local):
            for t in range(turns * cycles):
                rspread[t, s * TILE : (s + 1) * TILE] = right_ref[
                    s, h * TILE : (h + 1) * TILE, t * LANES : (t + 1) * LANES
                ].astype(jnp.float32)

        def pack(step, carry, h=h):
            chunk, cycle = step // cycles, lax.rem(step, cycles)
            tiles = [
                [
                    rspread[
                        cycle * turns + t,
                        pl.ds(chunk * period + e, local, stride=TILE),
                    ].astype(jnp.bfloat16)
                    for t in range(turns)
                ]
                for e in range(period)
            ]
            for d, outs in enumerate(pack_columns(cols, period, tiles)):
                for u, out in enumerate(outs):
                    sbuf[
                        h * per_half + chunk, cycle * period + d, :,
                        u * LANES : (u + 1) * LANES,
                    ] = out
            return carry

        lax.fori_loop(0, per_half * cycles, pack, 0)

    def rcopy(chunk, to, slot):
        return pltpu.make_async_remote_copy(
            src_ref=sbuf.at[chunk, to],
            dst_ref=rbuf.at[chunk, slot],
            send_sem=rsend.at[chunk, to],
            recv_sem=rrecv.at[chunk, slot],
            device_id={"col": to},
            device_id_type=MESH,
        )

    def lcopy(slot, to, send):
        return pltpu.make_async_remote_copy(
            src_ref=lbuf.at[slot],
            dst_ref=lbuf.at[slot],
            send_sem=lsend.at[send],
            recv_sem=lrecv.at[slot],
            device_id={"col": to},
            device_id_type=MESH,
        )

    pl.semaphore_wait(barrier, n - 1)

    mates = [base + lax.rem(me - base + 2 * j, half) for j in range(1, half // 2)]
    sources = [base + lax.rem(me - base + half - 2 * j, half) for j in range(1, half // 2)]
    sends = []

    def send_left(slot, to):
        copy = lcopy(slot, to, len(sends))
        copy.start()
        sends.append(copy)

    def other(slot):
        return lax.rem(slot + half, n)

    for to in [mirror] + mates + [partner]:
        send_left(me, to)
    for chunk in range(chunks):

        def send_right(k, carry, chunk=chunk):
            to = lax.rem(me + k, n)
            rcopy(chunk, to, me).start()
            return carry

        lax.fori_loop(1, n, send_right, 0)

    fetch_weight.wait()
    fetch_bias.wait()
    for start in range(0, channels, LANES):
        chosen = swap_matrix(width, width, start, LANES, channels)
        block = jnp.dot(chosen, weight_ref[...], preferred_element_type=jnp.float32)
        wturn[:, start : start + LANES] = block.T.astype(jnp.bfloat16)

    lcopy(mirror, me, 0).wait_recv()
    for to in mates + [partner]:
        send_left(mirror, to)
    for source in sources:
        for slot in (source, other(source)):
            lcopy(slot, me, 0).wait_recv()
            send_left(slot, partner)
    for j in range(half // 2):
        slot = base + lax.rem(partner - base + 2 * j, half)
        for slot in (slot, other(slot)):
            lcopy(slot, me, 0).wait_recv()
    for s in range(0, n, LANES // TILE):
        block = jnp.concatenate([lbuf[s + p] for p in range(LANES // TILE)], axis=0)
        lturn[:, s * TILE : s * TILE + LANES] = block.T

    def place(slot, block):
        start = pl.multiple_of(slot * TILE, TILE)
        for e, wide in enumerate(unpack_columns(cols, period, block)):
            rwide[pl.ds(start, TILE), e * LANES : (e + 1) * LANES] = wide

    def multiply(step, carry):
        lanes = pl.ds(pl.multiple_of(step * 2 * LANES, 2 * LANES), 2 * LANES)
        product = jnp.dot(
            lturn[...], rwide[:, lanes], preferred_element_type=jnp.float32
        ).astype(jnp.bfloat16)
        for side_e in range(2):
            at = pl.ds(pl.multiple_of((step * 2 + side_e) * width, width), width)
            for i in range(rows):
                side = (i % 2) * LANES
                flat[i // 2, at, side : side + LANES] = product[
                    i * width : (i + 1) * width, side_e * LANES : (side_e + 1) * LANES
                ]
        return carry

    for chunk in range(chunks):
        place(me, [sbuf[chunk, me, :, u * LANES : (u + 1) * LANES] for u in range(turns)])

        def arrive(k, carry, chunk=chunk):
            slot = lax.rem(me + n - k, n)
            rcopy(chunk, slot, slot).wait_recv()
            place(slot, [rbuf[chunk, slot, :, u * LANES : (u + 1) * LANES] for u in range(turns)])
            return carry

        lax.fori_loop(1, n, arrive, 0)
        lax.fori_loop(0, period // 2, multiply, 0)

        def project(pair, carry, chunk=chunk):
            for step in (2 * pair, 2 * pair + 1):
                update = jnp.dot(
                    wturn[:, chunk * deep : (chunk + 1) * deep], flat[step],
                    preferred_element_type=jnp.float32,
                )
                if chunk:
                    update = update + partial[step]
                if chunk < chunks - 1:
                    partial[step] = update
                else:
                    update = update.T * (1.0 / seqs) + bias_ref[...]
                    update = update.astype(out_ref.dtype)
                    out_ref[2 * step] = update[:cols]
                    out_ref[2 * step + 1] = update[LANES : LANES + cols]
            return carry

        lax.fori_loop(0, rows // 4, project, 0)

    for chunk in range(chunks):

        def sent(k, carry, chunk=chunk):
            rcopy(chunk, lax.rem(me + k, n), me).wait_send()
            return carry

        lax.fori_loop(1, n, sent, 0)
    for copy in sends:
        copy.wait_send()


def packed_call(n, left, right, out_weight, out_bias):
    local, rows, width = left.shape
    cols = right.shape[1] // n
    pair = out_weight.shape[1]
    seqs = local * n
    period = LANES // math.gcd(cols, LANES)
    chunks = width // period
    lanes = cols * period
    hbm = pl.BlockSpec(memory_space=pltpu.HBM)
    vmem = pl.BlockSpec(memory_space=pltpu.VMEM)
    dma = pltpu.SemaphoreType.DMA
    bf16, f32 = jnp.bfloat16, jnp.float32
    return pl.pallas_call(
        functools.partial(packed_kernel, n, cols, period),
        out_shape=jax.ShapeDtypeStruct((rows, cols, pair), bf16),
        in_specs=[hbm] * 4,
        out_specs=vmem,
        scratch_shapes=[
            pltpu.VMEM((local, rows, width), bf16),
            pltpu.VMEM((local, width, n * cols), bf16),
            pltpu.VMEM((width * width, pair), bf16),
            pltpu.VMEM((1, pair), f32),
            pltpu.VMEM((local * rows, LANES), f32),
            pltpu.VMEM((n * cols // LANES, local * TILE, LANES), f32),
            pltpu.VMEM((chunks, n, local, lanes), bf16),
            pltpu.VMEM((chunks, n, local, lanes), bf16),
            pltpu.VMEM((n, local, rows * width), bf16),
            pltpu.VMEM((seqs, period * LANES), bf16),
            pltpu.VMEM((rows * width, seqs), bf16),
            pltpu.VMEM((pair, width * width), bf16),
            pltpu.VMEM((rows // 2, period * width, 2 * LANES), bf16),
            pltpu.VMEM((rows // 2, pair, 2 * LANES), f32),
            dma((chunks, n)), dma((chunks, n)), dma((n,)), dma((n,)),
            dma((3 + width // TILE,)),
        ],
        compiler_params=pltpu.CompilerParams(
            collective_id=0, has_side_effects=True, vmem_limit_bytes=28 * 1024 * 1024
        ),
    )(left, jnp.transpose(right, (0, 2, 1)), out_weight, out_bias.reshape(1, pair))


def packs(n, left, right):
    local, rows, width = left.shape
    cols = right.shape[1] // n
    period = LANES // math.gcd(cols, LANES)
    return (
        local == TILE and cols <= LANES and rows % 4 == 0 and rows <= 32
        and LANES % width == 0 and rows % (LANES // width) == 0
        and width % TILE == 0 and TILE % period == 0 and period % 2 == 0
        and n % period == 0 and n % (LANES // TILE) == 0 and n % 4 == 0
    )


def flip(x_ref, o_ref, h):
    chunks, columns, lanes = o_ref.shape
    part = x_ref.shape[1] // chunks
    step = 2 * LANES
    for start in range(0, columns, step):
        piece = x_ref[:, h * part : (h + 1) * part, start : start + step]
        o_ref[h, start : start + step] = piece.reshape(lanes, step).T


def swap_matrix(first, minor, start, rows, columns):
    row = lax.broadcasted_iota(jnp.int32, (rows, columns), 0) + start
    column = lax.broadcasted_iota(jnp.int32, (rows, columns), 1)
    shift = first.bit_length() - 1
    wanted = (row & (first - 1)) * minor + (row >> shift)
    return jnp.where(column == wanted, 1.0, 0.0).astype(jnp.bfloat16)


def kernel(
    n, width, cols, rows, chunks, given_ref, left_ref, weight_ref, bias_ref, out_ref,
    right_ref, rbuf, lbuf, rwide, lturn, wturn, flat, partial,
    rsend, rrecv, lsend, lrecv, fsend, own,
):
    me = lax.axis_index("col")
    place = lax.rem(me, GROUP)
    mates = [me - place + lax.rem(place + j, GROUP) for j in range(1, GROUP)]
    hops = n // GROUP
    local = left_ref.shape[0]
    seqs = n * local
    part = width // chunks

    def rcopy(h, k):
        to = lax.rem(me + k, n)
        start = pl.multiple_of(to * cols, TILE)
        return pltpu.make_async_remote_copy(
            src_ref=right_ref.at[h, pl.ds(start, cols)],
            dst_ref=rbuf.at[h, me],
            send_sem=rsend.at[h, k],
            recv_sem=rrecv.at[h, me],
            device_id={"col": to},
            device_id_type=MESH,
        )

    def lcopy(src, slot, to, send):
        return pltpu.make_async_remote_copy(
            src_ref=src,
            dst_ref=lbuf.at[slot],
            send_sem=send,
            recv_sem=lrecv.at[slot],
            device_id={"col": to},
            device_id_type=MESH,
        )

    barrier = pltpu.get_barrier_semaphore()
    for k in range(1, n):
        pl.semaphore_signal(
            barrier, inc=1, device_id={"col": lax.rem(me + k, n)}, device_id_type=MESH
        )
    flip(given_ref, right_ref, 0)
    pl.semaphore_wait(barrier, n - 1)

    sends = []
    for k in range(1, hops):
        sends.append(lcopy(left_ref, me, lax.rem(me + GROUP * k, n), lsend.at[k]))
    for j, mate in enumerate(mates):
        sends.append(lcopy(left_ref, me, mate, fsend.at[0, j]))
    for k in range(1, n):
        sends.append(rcopy(0, k))
    for copy in sends:
        copy.start()
    for h in range(1, chunks):
        flip(given_ref, right_ref, h)
    mine_left = pltpu.make_async_copy(left_ref, lbuf.at[me], own.at[chunks])
    mine_left.start()

    rwide[...] = jnp.zeros_like(rwide)
    channels = width * width
    for start in range(0, channels, LANES):
        chosen = swap_matrix(width, width, start, LANES, channels)
        block = jnp.dot(chosen, weight_ref[...], preferred_element_type=jnp.float32)
        wturn[:, start : start + LANES] = block.T.astype(jnp.bfloat16)
    for h in range(1, chunks):
        later = [rcopy(h, k) for k in range(1, n)]
        for copy in later:
            copy.start()
        sends += later
    mine = []
    for h in range(chunks):
        block = right_ref.at[h, pl.ds(pl.multiple_of(me * cols, TILE), cols)]
        mine.append(pltpu.make_async_copy(block, rbuf.at[h, me], own.at[h]))
        mine[h].start()
    swap = swap_matrix(TILE, part, 0, TILE * part, TILE * part)

    forwards = []
    for k in range(1, hops):
        slot = lax.rem(me + n - GROUP * k, n)
        lcopy(left_ref, slot, mates[0], lsend.at[k]).wait_recv()
        for j, mate in enumerate(mates):
            forward = lcopy(lbuf.at[slot], slot, mate, fsend.at[k, j])
            forward.start()
            forwards.append(forward)
    for k in range(hops):
        for j, mate in enumerate(mates):
            slot = lax.rem(mate + n - GROUP * k, n)
            lcopy(left_ref, slot, mate, fsend.at[k, j]).wait_recv()
    mine_left.wait()
    per = TILE // local
    blocks = []
    for group in range(seqs // TILE):
        parts = [lbuf[group * per + p] for p in range(per)]
        if per > 1:
            parts = [piece.astype(jnp.float32) for piece in parts]
            blocks.append(jnp.concatenate(parts, axis=0).astype(jnp.bfloat16))
        else:
            blocks.append(parts[0])
    lturn[...] = jnp.concatenate(blocks, axis=0).T

    def turn(h, start, block):
        turned = lax.dot_general(
            swap, block, (((1,), (1,)), ((), ())), preferred_element_type=jnp.float32
        ).astype(jnp.bfloat16)
        for e in range(part):
            at = (h * part + e) * LANES
            rwide[pl.ds(start, TILE), at : at + cols] = turned[e * TILE : (e + 1) * TILE]

    def arrive(h):
        def one(k, carry):
            slot = lax.rem(me + n - k, n)
            pltpu.make_async_remote_copy(
                src_ref=right_ref.at[h, pl.ds(0, cols)],
                dst_ref=rbuf.at[h, slot],
                send_sem=rsend.at[h, k],
                recv_sem=rrecv.at[h, slot],
                device_id={"col": slot},
                device_id_type=MESH,
            ).wait_recv()
            if per == 1:
                turn(h, pl.multiple_of(slot * TILE, TILE), rbuf[h, slot])
            return carry

        mine[h].wait()
        if per == 1:
            turn(h, pl.multiple_of(me * TILE, TILE), rbuf[h, me])
        lax.fori_loop(1, n, one, 0)
        if per > 1:
            for group in range(seqs // TILE):
                parts = [rbuf[h, group * per + p] for p in range(per)]
                turn(h, group * TILE, jnp.concatenate(parts, axis=1))

    count = flat.shape[0] * 2

    def multiply(base, h):
        def outer(step, carry):
            lanes = pl.ds(pl.multiple_of(step * 2 * LANES, 2 * LANES), 2 * LANES)
            product = jnp.dot(
                lturn[base * width : (base + count) * width, :],
                rwide[:, lanes],
                preferred_element_type=jnp.float32,
            ).astype(jnp.bfloat16)
            for side_e in range(2):
                at = pl.ds(pl.multiple_of((step * 2 + side_e) * width, width), width)
                for i in range(count):
                    side = (i % 2) * LANES
                    flat[i // 2, at, side : side + LANES] = product[
                        i * width : (i + 1) * width, side_e * LANES : (side_e + 1) * LANES
                    ]
            return carry

        lax.fori_loop(h * part // 2, (h + 1) * part // 2, outer, 0)

    deep = part * width
    early = rows == count and chunks > 1

    def project_early(step, carry):
        partial[step] = jnp.dot(
            wturn[:, : channels - deep],
            flat[step, : channels - deep],
            preferred_element_type=jnp.float32,
        )
        return carry

    for h in range(chunks):
        arrive(h)
        if rows == count:
            multiply(0, h)
        if early and h == chunks - 2:
            lax.fori_loop(0, count // 2, project_early, 0)

    skip = channels - deep if early else 0
    for base in range(0, rows, count):
        if rows != count:
            for h in range(chunks):
                multiply(base, h)

        def project(step, carry):
            update = jnp.dot(
                wturn[:, skip:], flat[step, skip:], preferred_element_type=jnp.float32
            )
            if early:
                update = update + partial[step]
            update = update.T * (1.0 / seqs) + bias_ref[...]
            update = update.astype(out_ref.dtype)
            out_ref[base + 2 * step] = update[:cols]
            out_ref[base + 2 * step + 1] = update[LANES : LANES + cols]
            return carry

        lax.fori_loop(0, count // 2, project, 0)

    for copy in sends + forwards:
        copy.wait_send()


def on_device(n, left, right, out_weight, out_bias):
    if packs(n, left, right):
        return packed_call(n, left, right, out_weight, out_bias)
    local, rows, width = left.shape
    cols = right.shape[1] // n
    pair = out_weight.shape[1]
    seqs = local * n
    chunks = 2 if local * width % (4 * LANES) == 0 else 1
    rows_step = min(rows, 32)
    vmem = pl.BlockSpec(memory_space=pltpu.VMEM)
    dma = pltpu.SemaphoreType.DMA
    return pl.pallas_call(
        functools.partial(kernel, n, width, cols, rows, chunks),
        out_shape=jax.ShapeDtypeStruct((rows, cols, pair), jnp.bfloat16),
        in_specs=[vmem] * 4,
        out_specs=vmem,
        scratch_shapes=[
            pltpu.VMEM((chunks, right.shape[1], local * width // chunks), jnp.bfloat16),
            pltpu.VMEM((chunks, n, cols, local * width // chunks), jnp.bfloat16),
            pltpu.VMEM((n, local, rows * width), jnp.bfloat16),
            pltpu.VMEM((seqs, width * LANES), jnp.bfloat16),
            pltpu.VMEM((rows * width, seqs), jnp.bfloat16),
            pltpu.VMEM((pair, width * width), jnp.bfloat16),
            pltpu.VMEM((rows_step // 2, width * width, 2 * LANES), jnp.bfloat16),
            pltpu.VMEM((rows_step // 2, pair, 2 * LANES), jnp.float32),
            dma((chunks, n)), dma((chunks, n)),
            dma((n // GROUP,)), dma((n,)), dma((n // GROUP, GROUP)), dma((chunks + 1,)),
        ],
        compiler_params=pltpu.CompilerParams(
            collective_id=0, has_side_effects=True, vmem_limit_bytes=60 * 1024 * 1024
        ),
    )(jnp.transpose(right, (0, 2, 1)), left.reshape(local, rows * width), out_weight, out_bias.reshape(1, pair))


def solution(mesh):
    return jax.shard_map(
        functools.partial(on_device, mesh.shape["col"]),
        mesh=mesh,
        in_specs=(P("col", "groups", None), P("col", "groups", None), P(), P()),
        out_specs=P("groups", "col", None),
        check_vma=False,
    )
```

```python
import functools
import math

import jax
import jax.numpy as jnp
from jax import lax
from jax.experimental import pallas as pl
from jax.experimental.pallas import tpu as pltpu
from jax.sharding import PartitionSpec as P

MESH = pl.DeviceIdType.MESH
LANES = 128
TILE = 16
GROUP = 4


def lane_index():
    return lax.broadcasted_iota(jnp.int32, (TILE, LANES), 1)


def turn_lanes(x, shift):
    shift %= LANES
    return pltpu.roll(x, shift, axis=1) if shift else x


def pick(lane, start, left, right):
    return jnp.where(lane >= start, right, left)


def pack_columns(cols, period, tiles):
    lane = lane_index()
    packed = []
    for d in range(period):
        first, offset = divmod(cols * d, LANES)
        moved = []
        for e in range(period):
            piece = tiles[e][first]
            if offset + cols > LANES:
                piece = pick(lane, offset, tiles[e][first + 1], piece)
            moved.append(turn_lanes(piece, cols * e - offset))
        outs = []
        for u in range(cols * period // LANES):
            low, high = u * LANES, (u + 1) * LANES
            out = None
            for e in range(period):
                start = cols * e
                if start + cols <= low or start >= high:
                    continue
                out = moved[e] if out is None else pick(lane, start - low, out, moved[e])
            outs.append(out)
        packed.append(outs)
    return packed


def unpack_columns(cols, period, tiles):
    lane = lane_index()
    wide = []
    for e in range(period):
        first, offset = divmod(cols * e, LANES)
        piece = tiles[first]
        if offset + cols > LANES:
            piece = pick(lane, offset, tiles[first + 1], piece)
        wide.append(turn_lanes(piece, -offset))
    return wide


def packed_kernel(
    n, cols, period, left_hbm, right_hbm, weight_hbm, bias_hbm, out_ref,
    left_ref, right_ref, weight_ref, bias_ref, lspread, rspread, sbuf, rbuf, lbuf,
    rwide, lturn, wturn, flat, partial,
    rsend, rrecv, lsend, lrecv, loads,
):
    me = lax.axis_index("col")
    half = n // 2
    base = me // half * half
    partner = me + 1 - 2 * lax.rem(me, 2)
    mirror = lax.rem(me + half, n)
    local, rows, width = left_ref.shape
    seqs = n * local
    chunks = width // period
    halves = width // TILE
    per_half = chunks // halves
    channels = width * width
    deep = period * width

    barrier = pltpu.get_barrier_semaphore()
    for k in range(1, n):
        pl.semaphore_signal(
            barrier, inc=1, device_id={"col": lax.rem(me + k, n)}, device_id_type=MESH
        )
    fetch_left = pltpu.make_async_copy(left_hbm, left_ref, loads.at[0])
    fetch_weight = pltpu.make_async_copy(weight_hbm, weight_ref, loads.at[1])
    fetch_bias = pltpu.make_async_copy(bias_hbm, bias_ref, loads.at[2])
    fetch_right = [
        pltpu.make_async_copy(
            right_hbm.at[:, pl.ds(h * TILE, TILE)],
            right_ref.at[:, pl.ds(h * TILE, TILE)],
            loads.at[3 + h],
        )
        for h in range(halves)
    ]
    fetch_left.start()
    for fetch in fetch_right:
        fetch.start()
    fetch_weight.start()
    fetch_bias.start()

    fetch_left.wait()
    for s in range(local):
        lspread[s * rows : (s + 1) * rows, :width] = left_ref[s].astype(jnp.float32)
    lane = lane_index()
    join = LANES // width
    for t in range(rows // join):
        block = lspread[pl.ds(t * join, local, stride=rows), :]
        for k in range(1, join):
            piece = lspread[pl.ds(t * join + k, local, stride=rows), :]
            block = pick(lane, k * width, block, turn_lanes(piece, k * width))
        lbuf[me, :, t * LANES : (t + 1) * LANES] = block.astype(jnp.bfloat16)

    turns = cols * period // LANES
    cycles = n // period
    for h in range(halves):
        fetch_right[h].wait()
        for s in range(local):
            for t in range(turns * cycles):
                rspread[t, s * TILE : (s + 1) * TILE] = right_ref[
                    s, h * TILE : (h + 1) * TILE, t * LANES : (t + 1) * LANES
                ].astype(jnp.float32)

        def pack(step, carry, h=h):
            chunk, cycle = step // cycles, lax.rem(step, cycles)
            tiles = [
                [
                    rspread[
                        cycle * turns + t,
                        pl.ds(chunk * period + e, local, stride=TILE),
                    ].astype(jnp.bfloat16)
                    for t in range(turns)
                ]
                for e in range(period)
            ]
            for d, outs in enumerate(pack_columns(cols, period, tiles)):
                for u, out in enumerate(outs):
                    sbuf[
                        h * per_half + chunk, cycle * period + d, :,
                        u * LANES : (u + 1) * LANES,
                    ] = out
            return carry

        lax.fori_loop(0, per_half * cycles, pack, 0)

    def rcopy(chunk, to, slot):
        return pltpu.make_async_remote_copy(
            src_ref=sbuf.at[chunk, to],
            dst_ref=rbuf.at[chunk, slot],
            send_sem=rsend.at[chunk, to],
            recv_sem=rrecv.at[chunk, slot],
            device_id={"col": to},
            device_id_type=MESH,
        )

    def lcopy(slot, to, send):
        return pltpu.make_async_remote_copy(
            src_ref=lbuf.at[slot],
            dst_ref=lbuf.at[slot],
            send_sem=lsend.at[send],
            recv_sem=lrecv.at[slot],
            device_id={"col": to},
            device_id_type=MESH,
        )

    pl.semaphore_wait(barrier, n - 1)

    mates = [base + lax.rem(me - base + 2 * j, half) for j in range(1, half // 2)]
    sources = [base + lax.rem(me - base + half - 2 * j, half) for j in range(1, half // 2)]
    sends = []

    def send_left(slot, to):
        copy = lcopy(slot, to, len(sends))
        copy.start()
        sends.append(copy)

    def other(slot):
        return lax.rem(slot + half, n)

    for to in [mirror] + mates + [partner]:
        send_left(me, to)

    def send_chunk(chunk):
        def send_right(k, carry):
            to = lax.rem(me + k, n)
            rcopy(chunk, to, me).start()
            return carry

        lax.fori_loop(1, n, send_right, 0)

    send_chunk(0)
    fetch_weight.wait()
    fetch_bias.wait()
    for start in range(0, channels, LANES):
        chosen = swap_matrix(width, width, start, LANES, channels)
        block = jnp.dot(chosen, weight_ref[...], preferred_element_type=jnp.float32)
        wturn[:, start : start + LANES] = block.T.astype(jnp.bfloat16)

    lcopy(mirror, me, 0).wait_recv()
    for to in mates + [partner]:
        send_left(mirror, to)
    for chunk in range(1, chunks):
        send_chunk(chunk)
    for source in sources:
        for slot in (source, other(source)):
            lcopy(slot, me, 0).wait_recv()
            send_left(slot, partner)
    for j in range(half // 2):
        slot = base + lax.rem(partner - base + 2 * j, half)
        for slot in (slot, other(slot)):
            lcopy(slot, me, 0).wait_recv()
    for s in range(0, n, LANES // TILE):
        block = jnp.concatenate([lbuf[s + p] for p in range(LANES // TILE)], axis=0)
        lturn[:, s * TILE : s * TILE + LANES] = block.T

    def place(slot, block):
        start = pl.multiple_of(slot * TILE, TILE)
        for e, wide in enumerate(unpack_columns(cols, period, block)):
            rwide[pl.ds(start, TILE), e * LANES : (e + 1) * LANES] = wide

    def multiply(step, carry):
        lanes = pl.ds(pl.multiple_of(step * 2 * LANES, 2 * LANES), 2 * LANES)
        product = jnp.dot(
            lturn[...], rwide[:, lanes], preferred_element_type=jnp.float32
        ).astype(jnp.bfloat16)
        for side_e in range(2):
            at = pl.ds(pl.multiple_of((step * 2 + side_e) * width, width), width)
            for i in range(rows):
                side = (i % 2) * LANES
                flat[i // 2, at, side : side + LANES] = product[
                    i * width : (i + 1) * width, side_e * LANES : (side_e + 1) * LANES
                ]
        return carry

    for chunk in range(chunks):
        place(me, [sbuf[chunk, me, :, u * LANES : (u + 1) * LANES] for u in range(turns)])

        def arrive(k, carry, chunk=chunk):
            slot = lax.rem(me + n - k, n)
            rcopy(chunk, slot, slot).wait_recv()
            place(slot, [rbuf[chunk, slot, :, u * LANES : (u + 1) * LANES] for u in range(turns)])
            return carry

        lax.fori_loop(1, n, arrive, 0)
        lax.fori_loop(0, period // 2, multiply, 0)

        def project(pair, carry, chunk=chunk):
            for step in (2 * pair, 2 * pair + 1):
                update = jnp.dot(
                    wturn[:, chunk * deep : (chunk + 1) * deep], flat[step],
                    preferred_element_type=jnp.float32,
                )
                if chunk:
                    update = update + partial[step]
                if chunk < chunks - 1:
                    partial[step] = update
                else:
                    update = update.T * (1.0 / seqs) + bias_ref[...]
                    update = update.astype(out_ref.dtype)
                    out_ref[2 * step] = update[:cols]
                    out_ref[2 * step + 1] = update[LANES : LANES + cols]
            return carry

        lax.fori_loop(0, rows // 4, project, 0)

    for chunk in range(chunks):

        def sent(k, carry, chunk=chunk):
            rcopy(chunk, lax.rem(me + k, n), me).wait_send()
            return carry

        lax.fori_loop(1, n, sent, 0)
    for copy in sends:
        copy.wait_send()


def packed_call(n, left, right, out_weight, out_bias):
    local, rows, width = left.shape
    cols = right.shape[1] // n
    pair = out_weight.shape[1]
    seqs = local * n
    period = LANES // math.gcd(cols, LANES)
    chunks = width // period
    lanes = cols * period
    hbm = pl.BlockSpec(memory_space=pltpu.HBM)
    vmem = pl.BlockSpec(memory_space=pltpu.VMEM)
    dma = pltpu.SemaphoreType.DMA
    bf16, f32 = jnp.bfloat16, jnp.float32
    return pl.pallas_call(
        functools.partial(packed_kernel, n, cols, period),
        out_shape=jax.ShapeDtypeStruct((rows, cols, pair), bf16),
        in_specs=[hbm] * 4,
        out_specs=vmem,
        scratch_shapes=[
            pltpu.VMEM((local, rows, width), bf16),
            pltpu.VMEM((local, width, n * cols), bf16),
            pltpu.VMEM((width * width, pair), bf16),
            pltpu.VMEM((1, pair), f32),
            pltpu.VMEM((local * rows, LANES), f32),
            pltpu.VMEM((n * cols // LANES, local * TILE, LANES), f32),
            pltpu.VMEM((chunks, n, local, lanes), bf16),
            pltpu.VMEM((chunks, n, local, lanes), bf16),
            pltpu.VMEM((n, local, rows * width), bf16),
            pltpu.VMEM((seqs, period * LANES), bf16),
            pltpu.VMEM((rows * width, seqs), bf16),
            pltpu.VMEM((pair, width * width), bf16),
            pltpu.VMEM((rows // 2, period * width, 2 * LANES), bf16),
            pltpu.VMEM((rows // 2, pair, 2 * LANES), f32),
            dma((chunks, n)), dma((chunks, n)), dma((n,)), dma((n,)),
            dma((3 + width // TILE,)),
        ],
        compiler_params=pltpu.CompilerParams(
            collective_id=0, has_side_effects=True, vmem_limit_bytes=60 * 1024 * 1024
        ),
    )(left, jnp.transpose(right, (0, 2, 1)), out_weight, out_bias.reshape(1, pair))


def packs(n, left, right):
    local, rows, width = left.shape
    cols = right.shape[1] // n
    period = LANES // math.gcd(cols, LANES)
    return (
        local == TILE and cols <= LANES and rows % 4 == 0 and rows <= 32
        and LANES % width == 0 and rows % (LANES // width) == 0
        and width % TILE == 0 and TILE % period == 0 and period % 2 == 0
        and n % period == 0 and n % (LANES // TILE) == 0 and n % 4 == 0
    )


def flip(x_ref, o_ref, h):
    chunks, columns, lanes = o_ref.shape
    part = x_ref.shape[1] // chunks
    step = 2 * LANES
    for start in range(0, columns, step):
        piece = x_ref[:, h * part : (h + 1) * part, start : start + step]
        o_ref[h, start : start + step] = piece.reshape(lanes, step).T


def swap_matrix(first, minor, start, rows, columns):
    row = lax.broadcasted_iota(jnp.int32, (rows, columns), 0) + start
    column = lax.broadcasted_iota(jnp.int32, (rows, columns), 1)
    shift = first.bit_length() - 1
    wanted = (row & (first - 1)) * minor + (row >> shift)
    return jnp.where(column == wanted, 1.0, 0.0).astype(jnp.bfloat16)


def kernel(
    n, width, cols, rows, chunks, given_ref, left_ref, weight_ref, bias_ref, out_ref,
    right_ref, rbuf, lbuf, rwide, lturn, wturn, flat, partial,
    rsend, rrecv, lsend, lrecv, fsend, own,
):
    me = lax.axis_index("col")
    place = lax.rem(me, GROUP)
    mates = [me - place + lax.rem(place + j, GROUP) for j in range(1, GROUP)]
    hops = n // GROUP
    local = left_ref.shape[0]
    seqs = n * local
    part = width // chunks

    def rcopy(h, k):
        to = lax.rem(me + k, n)
        start = pl.multiple_of(to * cols, TILE)
        return pltpu.make_async_remote_copy(
            src_ref=right_ref.at[h, pl.ds(start, cols)],
            dst_ref=rbuf.at[h, me],
            send_sem=rsend.at[h, k],
            recv_sem=rrecv.at[h, me],
            device_id={"col": to},
            device_id_type=MESH,
        )

    def lcopy(src, slot, to, send):
        return pltpu.make_async_remote_copy(
            src_ref=src,
            dst_ref=lbuf.at[slot],
            send_sem=send,
            recv_sem=lrecv.at[slot],
            device_id={"col": to},
            device_id_type=MESH,
        )

    barrier = pltpu.get_barrier_semaphore()
    for k in range(1, n):
        pl.semaphore_signal(
            barrier, inc=1, device_id={"col": lax.rem(me + k, n)}, device_id_type=MESH
        )
    flip(given_ref, right_ref, 0)
    pl.semaphore_wait(barrier, n - 1)

    sends = []
    for k in range(1, hops):
        sends.append(lcopy(left_ref, me, lax.rem(me + GROUP * k, n), lsend.at[k]))
    for j, mate in enumerate(mates):
        sends.append(lcopy(left_ref, me, mate, fsend.at[0, j]))
    for k in range(1, n):
        sends.append(rcopy(0, k))
    for copy in sends:
        copy.start()
    for h in range(1, chunks):
        flip(given_ref, right_ref, h)
    mine_left = pltpu.make_async_copy(left_ref, lbuf.at[me], own.at[chunks])
    mine_left.start()

    rwide[...] = jnp.zeros_like(rwide)
    channels = width * width
    for start in range(0, channels, LANES):
        chosen = swap_matrix(width, width, start, LANES, channels)
        block = jnp.dot(chosen, weight_ref[...], preferred_element_type=jnp.float32)
        wturn[:, start : start + LANES] = block.T.astype(jnp.bfloat16)
    for h in range(1, chunks):
        later = [rcopy(h, k) for k in range(1, n)]
        for copy in later:
            copy.start()
        sends += later
    mine = []
    for h in range(chunks):
        block = right_ref.at[h, pl.ds(pl.multiple_of(me * cols, TILE), cols)]
        mine.append(pltpu.make_async_copy(block, rbuf.at[h, me], own.at[h]))
        mine[h].start()
    swap = swap_matrix(TILE, part, 0, TILE * part, TILE * part)

    forwards = []
    for k in range(1, hops):
        slot = lax.rem(me + n - GROUP * k, n)
        lcopy(left_ref, slot, mates[0], lsend.at[k]).wait_recv()
        for j, mate in enumerate(mates):
            forward = lcopy(lbuf.at[slot], slot, mate, fsend.at[k, j])
            forward.start()
            forwards.append(forward)
    for k in range(hops):
        for j, mate in enumerate(mates):
            slot = lax.rem(mate + n - GROUP * k, n)
            lcopy(left_ref, slot, mate, fsend.at[k, j]).wait_recv()
    mine_left.wait()
    per = TILE // local
    blocks = []
    for group in range(seqs // TILE):
        parts = [lbuf[group * per + p] for p in range(per)]
        if per > 1:
            parts = [piece.astype(jnp.float32) for piece in parts]
            blocks.append(jnp.concatenate(parts, axis=0).astype(jnp.bfloat16))
        else:
            blocks.append(parts[0])
    lturn[...] = jnp.concatenate(blocks, axis=0).T

    def turn(h, start, block):
        turned = lax.dot_general(
            swap, block, (((1,), (1,)), ((), ())), preferred_element_type=jnp.float32
        ).astype(jnp.bfloat16)
        for e in range(part):
            at = (h * part + e) * LANES
            rwide[pl.ds(start, TILE), at : at + cols] = turned[e * TILE : (e + 1) * TILE]

    def arrive(h):
        def one(k, carry):
            slot = lax.rem(me + n - k, n)
            pltpu.make_async_remote_copy(
                src_ref=right_ref.at[h, pl.ds(0, cols)],
                dst_ref=rbuf.at[h, slot],
                send_sem=rsend.at[h, k],
                recv_sem=rrecv.at[h, slot],
                device_id={"col": slot},
                device_id_type=MESH,
            ).wait_recv()
            if per == 1:
                turn(h, pl.multiple_of(slot * TILE, TILE), rbuf[h, slot])
            return carry

        mine[h].wait()
        if per == 1:
            turn(h, pl.multiple_of(me * TILE, TILE), rbuf[h, me])
        lax.fori_loop(1, n, one, 0)
        if per > 1:
            for group in range(seqs // TILE):
                parts = [rbuf[h, group * per + p] for p in range(per)]
                turn(h, group * TILE, jnp.concatenate(parts, axis=1))

    count = flat.shape[0] * 2

    def multiply(base, h):
        def outer(step, carry):
            lanes = pl.ds(pl.multiple_of(step * 2 * LANES, 2 * LANES), 2 * LANES)
            product = jnp.dot(
                lturn[base * width : (base + count) * width, :],
                rwide[:, lanes],
                preferred_element_type=jnp.float32,
            ).astype(jnp.bfloat16)
            for side_e in range(2):
                at = pl.ds(pl.multiple_of((step * 2 + side_e) * width, width), width)
                for i in range(count):
                    side = (i % 2) * LANES
                    flat[i // 2, at, side : side + LANES] = product[
                        i * width : (i + 1) * width, side_e * LANES : (side_e + 1) * LANES
                    ]
            return carry

        lax.fori_loop(h * part // 2, (h + 1) * part // 2, outer, 0)

    deep = part * width
    early = rows == count and chunks > 1

    def project_early(step, carry):
        partial[step] = jnp.dot(
            wturn[:, : channels - deep],
            flat[step, : channels - deep],
            preferred_element_type=jnp.float32,
        )
        return carry

    for h in range(chunks):
        arrive(h)
        if rows == count:
            multiply(0, h)
        if early and h == chunks - 2:
            lax.fori_loop(0, count // 2, project_early, 0)

    skip = channels - deep if early else 0
    for base in range(0, rows, count):
        if rows != count:
            for h in range(chunks):
                multiply(base, h)

        def project(step, carry):
            update = jnp.dot(
                wturn[:, skip:], flat[step, skip:], preferred_element_type=jnp.float32
            )
            if early:
                update = update + partial[step]
            update = update.T * (1.0 / seqs) + bias_ref[...]
            update = update.astype(out_ref.dtype)
            out_ref[base + 2 * step] = update[:cols]
            out_ref[base + 2 * step + 1] = update[LANES : LANES + cols]
            return carry

        lax.fori_loop(0, count // 2, project, 0)

    for copy in sends + forwards:
        copy.wait_send()


def on_device(n, left, right, out_weight, out_bias):
    if packs(n, left, right):
        return packed_call(n, left, right, out_weight, out_bias)
    local, rows, width = left.shape
    cols = right.shape[1] // n
    pair = out_weight.shape[1]
    seqs = local * n
    chunks = 2 if local * width % (4 * LANES) == 0 else 1
    rows_step = min(rows, 32)
    vmem = pl.BlockSpec(memory_space=pltpu.VMEM)
    dma = pltpu.SemaphoreType.DMA
    return pl.pallas_call(
        functools.partial(kernel, n, width, cols, rows, chunks),
        out_shape=jax.ShapeDtypeStruct((rows, cols, pair), jnp.bfloat16),
        in_specs=[vmem] * 4,
        out_specs=vmem,
        scratch_shapes=[
            pltpu.VMEM((chunks, right.shape[1], local * width // chunks), jnp.bfloat16),
            pltpu.VMEM((chunks, n, cols, local * width // chunks), jnp.bfloat16),
            pltpu.VMEM((n, local, rows * width), jnp.bfloat16),
            pltpu.VMEM((seqs, width * LANES), jnp.bfloat16),
            pltpu.VMEM((rows * width, seqs), jnp.bfloat16),
            pltpu.VMEM((pair, width * width), jnp.bfloat16),
            pltpu.VMEM((rows_step // 2, width * width, 2 * LANES), jnp.bfloat16),
            pltpu.VMEM((rows_step // 2, pair, 2 * LANES), jnp.float32),
            dma((chunks, n)), dma((chunks, n)),
            dma((n // GROUP,)), dma((n,)), dma((n // GROUP, GROUP)), dma((chunks + 1,)),
        ],
        compiler_params=pltpu.CompilerParams(
            collective_id=0, has_side_effects=True, vmem_limit_bytes=60 * 1024 * 1024
        ),
    )(jnp.transpose(right, (0, 2, 1)), left.reshape(local, rows * width), out_weight, out_bias.reshape(1, pair))


def solution(mesh):
    return jax.shard_map(
        functools.partial(on_device, mesh.shape["col"]),
        mesh=mesh,
        in_specs=(P("col", "groups", None), P("col", "groups", None), P(), P()),
        out_specs=P("groups", "col", None),
        check_vma=False,
    )
```

```python
import functools
import math

import jax
import jax.numpy as jnp
from jax import lax
from jax.experimental import pallas as pl
from jax.experimental.pallas import tpu as pltpu
from jax.sharding import PartitionSpec as P

MESH = pl.DeviceIdType.MESH
LANES = 128
TILE = 16
GROUP = 4
LAYERS = 4


def lane_index():
    return lax.broadcasted_iota(jnp.int32, (TILE, LANES), 1)


def turn_lanes(x, shift):
    shift %= LANES
    return pltpu.roll(x, shift, axis=1) if shift else x


def pick(lane, start, left, right):
    return jnp.where(lane >= start, right, left)


def pack_columns(cols, period, tiles):
    lane = lane_index()
    packed = []
    for d in range(period):
        first, offset = divmod(cols * d, LANES)
        moved = []
        for e in range(period):
            piece = tiles[e][first]
            if offset + cols > LANES:
                piece = pick(lane, offset, tiles[e][first + 1], piece)
            moved.append(turn_lanes(piece, cols * e - offset))
        outs = []
        for u in range(cols * period // LANES):
            low, high = u * LANES, (u + 1) * LANES
            out = None
            for e in range(period):
                start = cols * e
                if start + cols <= low or start >= high:
                    continue
                out = moved[e] if out is None else pick(lane, start - low, out, moved[e])
            outs.append(out)
        packed.append(outs)
    return packed


def unpack_columns(cols, period, tiles):
    lane = lane_index()
    wide = []
    for e in range(period):
        first, offset = divmod(cols * e, LANES)
        piece = tiles[first]
        if offset + cols > LANES:
            piece = pick(lane, offset, tiles[first + 1], piece)
        wide.append(turn_lanes(piece, -offset))
    return wide


def packed_kernel(
    n, cols, period, left_hbm, right_hbm, weight_hbm, bias_hbm, out_ref,
    left_ref, right_ref, weight_ref, bias_ref, lspread, rspread, sbuf, rbuf, lbuf,
    rwide, lturn, wturn, flat, partial,
    rsend, rrecv, lsend, lrecv, loads,
):
    me = lax.axis_index("col")
    half, span = n // 2, n // LAYERS
    base = me // half * half
    layer = me // span
    partner = me + 1 - 2 * lax.rem(me, 2)

    def other(slot):
        return (LAYERS - 1 - slot // span) * span + lax.rem(slot, span)

    mirror = other(me)
    local, rows, width = left_ref.shape
    seqs = n * local
    chunks = width // period
    halves = width // TILE
    per_half = chunks // halves
    channels = width * width
    deep = period * width

    barrier = pltpu.get_barrier_semaphore()
    for k in range(1, n):
        pl.semaphore_signal(
            barrier, inc=1, device_id={"col": lax.rem(me + k, n)}, device_id_type=MESH
        )
    fetch_left = pltpu.make_async_copy(left_hbm, left_ref, loads.at[0])
    fetch_weight = pltpu.make_async_copy(weight_hbm, weight_ref, loads.at[1])
    fetch_bias = pltpu.make_async_copy(bias_hbm, bias_ref, loads.at[2])
    fetch_right = [
        pltpu.make_async_copy(
            right_hbm.at[:, pl.ds(h * TILE, TILE)],
            right_ref.at[:, pl.ds(h * TILE, TILE)],
            loads.at[3 + h],
        )
        for h in range(halves)
    ]
    fetch_left.start()
    for fetch in fetch_right:
        fetch.start()
    fetch_weight.start()
    fetch_bias.start()

    fetch_left.wait()
    for s in range(local):
        lspread[s * rows : (s + 1) * rows, :width] = left_ref[s].astype(jnp.float32)
    lane = lane_index()
    join = LANES // width
    for t in range(rows // join):
        block = lspread[pl.ds(t * join, local, stride=rows), :]
        for k in range(1, join):
            piece = lspread[pl.ds(t * join + k, local, stride=rows), :]
            block = pick(lane, k * width, block, turn_lanes(piece, k * width))
        lbuf[me, :, t * LANES : (t + 1) * LANES] = block.astype(jnp.bfloat16)

    turns = cols * period // LANES
    cycles = n // period
    for h in range(halves):
        fetch_right[h].wait()
        for s in range(local):
            for t in range(turns * cycles):
                rspread[t, s * TILE : (s + 1) * TILE] = right_ref[
                    s, h * TILE : (h + 1) * TILE, t * LANES : (t + 1) * LANES
                ].astype(jnp.float32)

        def pack(step, carry, h=h):
            chunk, cycle = step // cycles, lax.rem(step, cycles)
            tiles = [
                [
                    rspread[
                        cycle * turns + t,
                        pl.ds(chunk * period + e, local, stride=TILE),
                    ].astype(jnp.bfloat16)
                    for t in range(turns)
                ]
                for e in range(period)
            ]
            for d, outs in enumerate(pack_columns(cols, period, tiles)):
                for u, out in enumerate(outs):
                    sbuf[
                        h * per_half + chunk, cycle * period + d, :,
                        u * LANES : (u + 1) * LANES,
                    ] = out
            return carry

        lax.fori_loop(0, per_half * cycles, pack, 0)

    def rcopy(chunk, to, slot):
        return pltpu.make_async_remote_copy(
            src_ref=sbuf.at[chunk, to],
            dst_ref=rbuf.at[chunk, slot],
            send_sem=rsend,
            recv_sem=rrecv.at[chunk, slot // span],
            device_id={"col": to},
            device_id_type=MESH,
        )

    def arrival(chunk, source, count):
        slots = pl.ds(source * span, count)
        return pltpu.make_async_remote_copy(
            src_ref=sbuf.at[chunk, slots],
            dst_ref=rbuf.at[chunk, slots],
            send_sem=rsend,
            recv_sem=rrecv.at[chunk, source],
            device_id={"col": mirror},
            device_id_type=MESH,
        )

    def lcopy(slot, to):
        return pltpu.make_async_remote_copy(
            src_ref=lbuf.at[slot],
            dst_ref=lbuf.at[slot],
            send_sem=lsend,
            recv_sem=lrecv.at[slot],
            device_id={"col": to},
            device_id_type=MESH,
        )

    own = pltpu.make_async_copy(sbuf.at[:, me], rbuf.at[:, me], loads.at[0])
    own.start()
    pl.semaphore_wait(barrier, n - 1)

    mates = [base + lax.rem(me - base + 2 * j, half) for j in range(1, half // 2)]
    sources = [base + lax.rem(me - base + half - 2 * j, half) for j in range(1, half // 2)]
    sends = []

    def send_left(slot, to):
        copy = lcopy(slot, to)
        copy.start()
        sends.append(copy)

    for to in [mirror] + mates + [partner]:
        send_left(me, to)

    def send_chunk(chunk):
        def send_right(k, carry):
            to = lax.rem(me + k, n)
            rcopy(chunk, to, me).start()
            return carry

        lax.fori_loop(1, n, send_right, 0)

    send_chunk(0)
    fetch_weight.wait()
    fetch_bias.wait()
    for start in range(0, channels, LANES):
        chosen = swap_matrix(width, width, start, LANES, channels)
        block = jnp.dot(chosen, weight_ref[...], preferred_element_type=jnp.float32)
        wturn[:, start : start + LANES] = block.T.astype(jnp.bfloat16)

    lcopy(mirror, me).wait_recv()
    for to in mates + [partner]:
        send_left(mirror, to)
    for chunk in range(1, chunks):
        send_chunk(chunk)
    for source in sources:
        for slot in (source, other(source)):
            lcopy(slot, me).wait_recv()
            send_left(slot, partner)
    for j in range(half // 2):
        slot = base + lax.rem(partner - base + 2 * j, half)
        for slot in (slot, other(slot)):
            lcopy(slot, me).wait_recv()
    for s in range(0, n, LANES // TILE):
        block = jnp.concatenate([lbuf[s + p] for p in range(LANES // TILE)], axis=0)
        lturn[:, s * TILE : s * TILE + LANES] = block.T

    def place(chunk, source):
        for p in range(span):
            slot = source * span + p
            start = pl.multiple_of(slot * TILE, TILE)
            block = [rbuf[chunk, slot, :, u * LANES : (u + 1) * LANES] for u in range(turns)]
            for e, wide in enumerate(unpack_columns(cols, period, block)):
                rwide[pl.ds(start, TILE), e * LANES : (e + 1) * LANES] = wide

    def multiply(step):
        lanes = slice(step * 2 * LANES, (step + 1) * 2 * LANES)
        product = jnp.dot(
            lturn[...], rwide[:, lanes], preferred_element_type=jnp.float32
        ).astype(jnp.bfloat16)
        for side_e in range(2):
            at = (step * 2 + side_e) * width
            for i in range(rows):
                side = (i % 2) * LANES
                flat[i // 2, at : at + width, side : side + LANES] = product[
                    i * width : (i + 1) * width, side_e * LANES : (side_e + 1) * LANES
                ]

    def project(chunk, step):
        update = jnp.dot(
            wturn[:, chunk * deep : (chunk + 1) * deep], flat[step],
            preferred_element_type=jnp.float32,
        )
        if chunk:
            update = update + partial[step]
        if chunk < chunks - 1:
            partial[step] = update
            return
        update = update.T * (1.0 / seqs) + bias_ref[...]
        update = update.astype(out_ref.dtype)
        out_ref[2 * step] = update[:cols]
        out_ref[2 * step + 1] = update[LANES : LANES + cols]

    low = layer < LAYERS // 2
    sibling = layer + 1 - 2 * lax.rem(layer, 2)
    outer = jnp.where(low, LAYERS - 1, 0)
    inner = jnp.where(low, LAYERS // 2, LAYERS // 2 - 1)
    own.wait()
    for chunk in range(chunks):
        arrival(chunk, layer, span - 1).wait_recv()
        place(chunk, layer)
        for source in (sibling, outer, inner):
            arrival(chunk, source, span).wait_recv()
            place(chunk, source)
        for step in range(period // 2):
            multiply(step)
        for step in range(rows // 2):
            project(chunk, step)

    pltpu.make_async_remote_copy(
        src_ref=sbuf.at[:, pl.ds(0, n - 1)],
        dst_ref=rbuf.at[:, pl.ds(0, n - 1)],
        send_sem=rsend,
        recv_sem=rrecv.at[0, 0],
        device_id={"col": mirror},
        device_id_type=MESH,
    ).wait_send()
    pltpu.make_async_remote_copy(
        src_ref=lbuf.at[pl.ds(0, len(sends))],
        dst_ref=lbuf.at[pl.ds(0, len(sends))],
        send_sem=lsend,
        recv_sem=lrecv.at[0],
        device_id={"col": mirror},
        device_id_type=MESH,
    ).wait_send()


def packed_call(n, left, right, out_weight, out_bias):
    local, rows, width = left.shape
    cols = right.shape[1] // n
    pair = out_weight.shape[1]
    seqs = local * n
    period = LANES // math.gcd(cols, LANES)
    chunks = width // period
    lanes = cols * period
    hbm = pl.BlockSpec(memory_space=pltpu.HBM)
    vmem = pl.BlockSpec(memory_space=pltpu.VMEM)
    dma = pltpu.SemaphoreType.DMA
    bf16, f32 = jnp.bfloat16, jnp.float32
    return pl.pallas_call(
        functools.partial(packed_kernel, n, cols, period),
        out_shape=jax.ShapeDtypeStruct((rows, cols, pair), bf16),
        in_specs=[hbm] * 4,
        out_specs=vmem,
        scratch_shapes=[
            pltpu.VMEM((local, rows, width), bf16),
            pltpu.VMEM((local, width, n * cols), bf16),
            pltpu.VMEM((width * width, pair), bf16),
            pltpu.VMEM((1, pair), f32),
            pltpu.VMEM((local * rows, LANES), f32),
            pltpu.VMEM((n * cols // LANES, local * TILE, LANES), f32),
            pltpu.VMEM((chunks, n, local, lanes), bf16),
            pltpu.VMEM((chunks, n, local, lanes), bf16),
            pltpu.VMEM((n, local, rows * width), bf16),
            pltpu.VMEM((seqs, period * LANES), bf16),
            pltpu.VMEM((rows * width, seqs), bf16),
            pltpu.VMEM((pair, width * width), bf16),
            pltpu.VMEM((rows // 2, period * width, 2 * LANES), bf16),
            pltpu.VMEM((rows // 2, pair, 2 * LANES), f32),
            dma(()), dma((chunks, LAYERS)), dma(()), dma((n,)),
            dma((3 + width // TILE,)),
        ],
        compiler_params=pltpu.CompilerParams(
            collective_id=0, has_side_effects=True, vmem_limit_bytes=40 * 1024 * 1024
        ),
    )(*(pltpu.with_memory_space_constraint(x, pltpu.HBM) for x in (left, jnp.transpose(right, (0, 2, 1)), out_weight, out_bias.reshape(1, pair))))


def packs(n, left, right):
    local, rows, width = left.shape
    cols = right.shape[1] // n
    period = LANES // math.gcd(cols, LANES)
    return (
        local == TILE and cols <= LANES and rows % 4 == 0 and rows <= 32
        and LANES % width == 0 and rows % (LANES // width) == 0
        and width % TILE == 0 and TILE % period == 0 and period % 2 == 0
        and n % period == 0 and n % (LANES // TILE) == 0 and n % 4 == 0
    )


def flip(x_ref, o_ref, h):
    chunks, columns, lanes = o_ref.shape
    part = x_ref.shape[1] // chunks
    step = 2 * LANES
    for start in range(0, columns, step):
        piece = x_ref[:, h * part : (h + 1) * part, start : start + step]
        o_ref[h, start : start + step] = piece.reshape(lanes, step).T


def swap_matrix(first, minor, start, rows, columns):
    row = lax.broadcasted_iota(jnp.int32, (rows, columns), 0) + start
    column = lax.broadcasted_iota(jnp.int32, (rows, columns), 1)
    shift = first.bit_length() - 1
    wanted = (row & (first - 1)) * minor + (row >> shift)
    return jnp.where(column == wanted, 1.0, 0.0).astype(jnp.bfloat16)


def kernel(
    n, width, cols, rows, chunks, given_ref, left_ref, weight_ref, bias_ref, out_ref,
    right_ref, rbuf, lbuf, rwide, lturn, wturn, flat, partial,
    rsend, rrecv, lsend, lrecv, fsend, own,
):
    me = lax.axis_index("col")
    place = lax.rem(me, GROUP)
    mates = [me - place + lax.rem(place + j, GROUP) for j in range(1, GROUP)]
    hops = n // GROUP
    local = left_ref.shape[0]
    seqs = n * local
    part = width // chunks

    def rcopy(h, k):
        to = lax.rem(me + k, n)
        start = pl.multiple_of(to * cols, TILE)
        return pltpu.make_async_remote_copy(
            src_ref=right_ref.at[h, pl.ds(start, cols)],
            dst_ref=rbuf.at[h, me],
            send_sem=rsend.at[h, k],
            recv_sem=rrecv.at[h, me],
            device_id={"col": to},
            device_id_type=MESH,
        )

    def lcopy(src, slot, to, send):
        return pltpu.make_async_remote_copy(
            src_ref=src,
            dst_ref=lbuf.at[slot],
            send_sem=send,
            recv_sem=lrecv.at[slot],
            device_id={"col": to},
            device_id_type=MESH,
        )

    barrier = pltpu.get_barrier_semaphore()
    for k in range(1, n):
        pl.semaphore_signal(
            barrier, inc=1, device_id={"col": lax.rem(me + k, n)}, device_id_type=MESH
        )
    flip(given_ref, right_ref, 0)
    pl.semaphore_wait(barrier, n - 1)

    sends = []
    for k in range(1, hops):
        sends.append(lcopy(left_ref, me, lax.rem(me + GROUP * k, n), lsend.at[k]))
    for j, mate in enumerate(mates):
        sends.append(lcopy(left_ref, me, mate, fsend.at[0, j]))
    for k in range(1, n):
        sends.append(rcopy(0, k))
    for copy in sends:
        copy.start()
    for h in range(1, chunks):
        flip(given_ref, right_ref, h)
    mine_left = pltpu.make_async_copy(left_ref, lbuf.at[me], own.at[chunks])
    mine_left.start()

    rwide[...] = jnp.zeros_like(rwide)
    channels = width * width
    for start in range(0, channels, LANES):
        chosen = swap_matrix(width, width, start, LANES, channels)
        block = jnp.dot(chosen, weight_ref[...], preferred_element_type=jnp.float32)
        wturn[:, start : start + LANES] = block.T.astype(jnp.bfloat16)
    for h in range(1, chunks):
        later = [rcopy(h, k) for k in range(1, n)]
        for copy in later:
            copy.start()
        sends += later
    mine = []
    for h in range(chunks):
        block = right_ref.at[h, pl.ds(pl.multiple_of(me * cols, TILE), cols)]
        mine.append(pltpu.make_async_copy(block, rbuf.at[h, me], own.at[h]))
        mine[h].start()
    swap = swap_matrix(TILE, part, 0, TILE * part, TILE * part)

    forwards = []
    for k in range(1, hops):
        slot = lax.rem(me + n - GROUP * k, n)
        lcopy(left_ref, slot, mates[0], lsend.at[k]).wait_recv()
        for j, mate in enumerate(mates):
            forward = lcopy(lbuf.at[slot], slot, mate, fsend.at[k, j])
            forward.start()
            forwards.append(forward)
    for k in range(hops):
        for j, mate in enumerate(mates):
            slot = lax.rem(mate + n - GROUP * k, n)
            lcopy(left_ref, slot, mate, fsend.at[k, j]).wait_recv()
    mine_left.wait()
    per = TILE // local
    blocks = []
    for group in range(seqs // TILE):
        parts = [lbuf[group * per + p] for p in range(per)]
        if per > 1:
            parts = [piece.astype(jnp.float32) for piece in parts]
            blocks.append(jnp.concatenate(parts, axis=0).astype(jnp.bfloat16))
        else:
            blocks.append(parts[0])
    lturn[...] = jnp.concatenate(blocks, axis=0).T

    def turn(h, start, block):
        turned = lax.dot_general(
            swap, block, (((1,), (1,)), ((), ())), preferred_element_type=jnp.float32
        ).astype(jnp.bfloat16)
        for e in range(part):
            at = (h * part + e) * LANES
            rwide[pl.ds(start, TILE), at : at + cols] = turned[e * TILE : (e + 1) * TILE]

    def arrive(h):
        def one(k, carry):
            slot = lax.rem(me + n - k, n)
            pltpu.make_async_remote_copy(
                src_ref=right_ref.at[h, pl.ds(0, cols)],
                dst_ref=rbuf.at[h, slot],
                send_sem=rsend.at[h, k],
                recv_sem=rrecv.at[h, slot],
                device_id={"col": slot},
                device_id_type=MESH,
            ).wait_recv()
            if per == 1:
                turn(h, pl.multiple_of(slot * TILE, TILE), rbuf[h, slot])
            return carry

        mine[h].wait()
        if per == 1:
            turn(h, pl.multiple_of(me * TILE, TILE), rbuf[h, me])
        lax.fori_loop(1, n, one, 0)
        if per > 1:
            for group in range(seqs // TILE):
                parts = [rbuf[h, group * per + p] for p in range(per)]
                turn(h, group * TILE, jnp.concatenate(parts, axis=1))

    count = flat.shape[0] * 2

    def multiply(base, h):
        def outer(step, carry):
            lanes = pl.ds(pl.multiple_of(step * 2 * LANES, 2 * LANES), 2 * LANES)
            product = jnp.dot(
                lturn[base * width : (base + count) * width, :],
                rwide[:, lanes],
                preferred_element_type=jnp.float32,
            ).astype(jnp.bfloat16)
            for side_e in range(2):
                at = pl.ds(pl.multiple_of((step * 2 + side_e) * width, width), width)
                for i in range(count):
                    side = (i % 2) * LANES
                    flat[i // 2, at, side : side + LANES] = product[
                        i * width : (i + 1) * width, side_e * LANES : (side_e + 1) * LANES
                    ]
            return carry

        lax.fori_loop(h * part // 2, (h + 1) * part // 2, outer, 0)

    deep = part * width
    early = rows == count and chunks > 1

    def project_early(step, carry):
        partial[step] = jnp.dot(
            wturn[:, : channels - deep],
            flat[step, : channels - deep],
            preferred_element_type=jnp.float32,
        )
        return carry

    for h in range(chunks):
        arrive(h)
        if rows == count:
            multiply(0, h)
        if early and h == chunks - 2:
            lax.fori_loop(0, count // 2, project_early, 0)

    skip = channels - deep if early else 0
    for base in range(0, rows, count):
        if rows != count:
            for h in range(chunks):
                multiply(base, h)

        def project(step, carry):
            update = jnp.dot(
                wturn[:, skip:], flat[step, skip:], preferred_element_type=jnp.float32
            )
            if early:
                update = update + partial[step]
            update = update.T * (1.0 / seqs) + bias_ref[...]
            update = update.astype(out_ref.dtype)
            out_ref[base + 2 * step] = update[:cols]
            out_ref[base + 2 * step + 1] = update[LANES : LANES + cols]
            return carry

        lax.fori_loop(0, count // 2, project, 0)

    for copy in sends + forwards:
        copy.wait_send()


def on_device(n, left, right, out_weight, out_bias):
    if packs(n, left, right):
        return packed_call(n, left, right, out_weight, out_bias)
    local, rows, width = left.shape
    cols = right.shape[1] // n
    pair = out_weight.shape[1]
    seqs = local * n
    chunks = 2 if local * width % (4 * LANES) == 0 else 1
    rows_step = min(rows, 32)
    vmem = pl.BlockSpec(memory_space=pltpu.VMEM)
    dma = pltpu.SemaphoreType.DMA
    return pl.pallas_call(
        functools.partial(kernel, n, width, cols, rows, chunks),
        out_shape=jax.ShapeDtypeStruct((rows, cols, pair), jnp.bfloat16),
        in_specs=[vmem] * 4,
        out_specs=vmem,
        scratch_shapes=[
            pltpu.VMEM((chunks, right.shape[1], local * width // chunks), jnp.bfloat16),
            pltpu.VMEM((chunks, n, cols, local * width // chunks), jnp.bfloat16),
            pltpu.VMEM((n, local, rows * width), jnp.bfloat16),
            pltpu.VMEM((seqs, width * LANES), jnp.bfloat16),
            pltpu.VMEM((rows * width, seqs), jnp.bfloat16),
            pltpu.VMEM((pair, width * width), jnp.bfloat16),
            pltpu.VMEM((rows_step // 2, width * width, 2 * LANES), jnp.bfloat16),
            pltpu.VMEM((rows_step // 2, pair, 2 * LANES), jnp.float32),
            dma((chunks, n)), dma((chunks, n)),
            dma((n // GROUP,)), dma((n,)), dma((n // GROUP, GROUP)), dma((chunks + 1,)),
        ],
        compiler_params=pltpu.CompilerParams(
            collective_id=0, has_side_effects=True, vmem_limit_bytes=40 * 1024 * 1024
        ),
    )(jnp.transpose(right, (0, 2, 1)), left.reshape(local, rows * width), out_weight, out_bias.reshape(1, pair))


def solution(mesh):
    return jax.shard_map(
        functools.partial(on_device, mesh.shape["col"]),
        mesh=mesh,
        in_specs=(P("col", "groups", None), P("col", "groups", None), P(), P()),
        out_specs=P("groups", "col", None),
        check_vma=False,
    )
```

```python
import functools
import math

import jax
import jax.numpy as jnp
from jax import lax
from jax.experimental import pallas as pl
from jax.experimental.pallas import tpu as pltpu
from jax.sharding import PartitionSpec as P

MESH = pl.DeviceIdType.MESH
LANES = 128
TILE = 16
GROUP = 4
LAYERS = 4


def lane_index():
    return lax.broadcasted_iota(jnp.int32, (TILE, LANES), 1)


def turn_lanes(x, shift):
    shift %= LANES
    return pltpu.roll(x, shift, axis=1) if shift else x


def pick(lane, start, left, right):
    return jnp.where(lane >= start, right, left)


def pack_columns(cols, period, tiles):
    lane = lane_index()
    packed = []
    for d in range(period):
        first, offset = divmod(cols * d, LANES)
        moved = []
        for e in range(period):
            piece = tiles[e][first]
            if offset + cols > LANES:
                piece = pick(lane, offset, tiles[e][first + 1], piece)
            moved.append(turn_lanes(piece, cols * e - offset))
        outs = []
        for u in range(cols * period // LANES):
            low, high = u * LANES, (u + 1) * LANES
            out = None
            for e in range(period):
                start = cols * e
                if start + cols <= low or start >= high:
                    continue
                out = moved[e] if out is None else pick(lane, start - low, out, moved[e])
            outs.append(out)
        packed.append(outs)
    return packed


def unpack_columns(cols, period, tiles):
    lane = lane_index()
    wide = []
    for e in range(period):
        first, offset = divmod(cols * e, LANES)
        piece = tiles[first]
        if offset + cols > LANES:
            piece = pick(lane, offset, tiles[first + 1], piece)
        wide.append(turn_lanes(piece, -offset))
    return wide


def packed_kernel(
    n, cols, period, left_hbm, right_hbm, weight_hbm, bias_hbm, out_ref,
    left_ref, right_ref, weight_ref, bias_ref, bias_turned, lspread, rspread, sbuf, rbuf, lbuf,
    rwide, lturn, wturn, flat, partial,
    rsend, rrecv, lsend, lrecv, loads, edges_in, layer_in, far_in, all_in,
):
    me = lax.axis_index("col")
    span = n // LAYERS
    layer, place_in = me // span, lax.rem(me, span)
    sibling = layer + 1 - 2 * lax.rem(layer, 2)
    low = layer < LAYERS // 2
    is_inner = (layer == LAYERS // 2 - 1) | (layer == LAYERS // 2)
    outer = jnp.where(low, LAYERS - 1, 0)
    inner = jnp.where(low, LAYERS // 2, LAYERS // 2 - 1)
    partner = me + 1 - 2 * lax.rem(me, 2)
    near = sibling * span + place_in

    def other(slot):
        return (LAYERS - 1 - slot // span) * span + lax.rem(slot, span)

    mirror = other(me)
    local, rows, width = left_ref.shape
    seqs = n * local
    chunks = width // period
    halves = width // TILE
    per_half = chunks // halves
    channels = width * width
    deep = period * width
    groups = [(0, per_half)] + [(chunk, 1) for chunk in range(per_half, chunks)]

    barrier = pltpu.get_barrier_semaphore()

    def greet(semaphore, to):
        pl.semaphore_signal(semaphore, inc=1, device_id={"col": to}, device_id_type=MESH)

    @pl.when(is_inner)
    def _():
        for p in range(span):
            greet(barrier, inner * span + p)
        for p in range(span):
            greet(barrier, sibling * span + p)

    fetch_left = pltpu.make_async_copy(left_hbm, left_ref, loads.at[0])
    fetch_weight = pltpu.make_async_copy(weight_hbm, weight_ref, loads.at[1])
    fetch_bias = pltpu.make_async_copy(bias_hbm, bias_ref, loads.at[2])
    fetch_right = [
        pltpu.make_async_copy(
            right_hbm.at[:, pl.ds(h * TILE, TILE)],
            right_ref.at[:, pl.ds(h * TILE, TILE)],
            loads.at[3 + h],
        )
        for h in range(halves)
    ]
    for fetch in fetch_right:
        fetch.start()
    fetch_left.start()
    fetch_weight.start()
    fetch_bias.start()

    turns = cols * period // LANES
    cycles = n // period

    def spread_half(h):
        fetch_right[h].wait()
        for s in range(local):
            for t in range(turns * cycles):
                rspread[t, s * TILE : (s + 1) * TILE] = right_ref[
                    s, h * TILE : (h + 1) * TILE, t * LANES : (t + 1) * LANES
                ].astype(jnp.float32)

    def pack_half(h, first, count):
        def pack(step, carry):
            chunk, cycle = step // count, first + lax.rem(step, count)
            tiles = [
                [
                    rspread[
                        cycle * turns + t,
                        pl.ds(chunk * period + e, local, stride=TILE),
                    ].astype(jnp.bfloat16)
                    for t in range(turns)
                ]
                for e in range(period)
            ]
            for d, outs in enumerate(pack_columns(cols, period, tiles)):
                for u, out in enumerate(outs):
                    sbuf[
                        h * per_half + chunk, cycle * period + d, :,
                        u * LANES : (u + 1) * LANES,
                    ] = out
            return carry

        lax.fori_loop(0, per_half * count, pack, 0)

    def send_right(group, to):
        first, count = groups[group]
        pltpu.make_async_remote_copy(
            src_ref=sbuf.at[pl.ds(first, count), to],
            dst_ref=rbuf.at[pl.ds(first, count), me],
            send_sem=rsend,
            recv_sem=rrecv.at[group, layer],
            device_id={"col": to},
            device_id_type=MESH,
        ).start()

    def send_layer(group, target, own=False):
        for p in range(int(own), span):
            send_right(group, target * span + lax.rem(place_in + p, span))

    def arrival(group, source, number):
        first, count = groups[group]
        slots = pl.ds(source * span, number)
        return pltpu.make_async_remote_copy(
            src_ref=sbuf.at[pl.ds(first, count), slots],
            dst_ref=rbuf.at[pl.ds(first, count), slots],
            send_sem=rsend,
            recv_sem=rrecv.at[group, source],
            device_id={"col": mirror},
            device_id_type=MESH,
        )

    def lcopy(slot, to):
        return pltpu.make_async_remote_copy(
            src_ref=lbuf.at[slot],
            dst_ref=lbuf.at[slot],
            send_sem=lsend,
            recv_sem=lrecv.at[slot],
            device_id={"col": to},
            device_id_type=MESH,
        )

    mates_near = [
        sibling * span + lax.rem(place_in + 2 * j, span) for j in range(span // 2)
    ]
    mates_own = [
        layer * span + lax.rem(place_in + 2 * j, span) for j in range(1, span // 2)
    ]
    mates = mates_near + mates_own

    half_cycles = cycles // 2
    mine = jnp.where(low, 0, half_cycles)
    theirs = half_cycles - mine
    early = jnp.where(is_inner, theirs, mine)
    spread_half(0)
    pack_half(0, early, half_cycles)
    pl.semaphore_wait(barrier, span)

    @pl.when(is_inner)
    def _():
        greet(layer_in, mirror)
        send_layer(0, inner)

    @pl.when(jnp.logical_not(is_inner))
    def _():
        for p in range(span):
            greet(edges_in, sibling * span + p)
        send_layer(0, sibling)

    pack_half(0, half_cycles - early, half_cycles)
    fetch_left.wait()
    for s in range(local):
        lspread[s * rows : (s + 1) * rows, :width] = left_ref[s].astype(jnp.float32)
    lane = lane_index()
    join = LANES // width
    for t in range(rows // join):
        block = lspread[pl.ds(t * join, local, stride=rows), :]
        for k in range(1, join):
            piece = lspread[pl.ds(t * join + k, local, stride=rows), :]
            block = pick(lane, k * width, block, turn_lanes(piece, k * width))
        lbuf[me, :, t * LANES : (t + 1) * LANES] = block.astype(jnp.bfloat16)

    @pl.when(is_inner)
    def _():
        pl.semaphore_wait(edges_in, span)
        pl.semaphore_wait(layer_in, 1)
        greet(far_in, mirror)
        for to in [mirror] + mates + [partner]:
            lcopy(me, to).start()
        send_layer(0, layer, own=True)
        send_layer(0, sibling)
        pl.semaphore_wait(far_in, 1)
        greet(all_in, near)
        send_layer(0, outer)

    @pl.when(jnp.logical_not(is_inner))
    def _():
        pl.semaphore_wait(all_in, 1)
        for to in [mirror] + mates + [partner]:
            lcopy(me, to).start()
        send_layer(0, layer, own=True)
        send_layer(0, inner)
        send_layer(0, outer)

    for h in range(1, halves):
        spread_half(h)
        pack_half(h, 0, cycles)
    own = pltpu.make_async_copy(sbuf.at[:, me], rbuf.at[:, me], loads.at[0])
    own.start()

    lcopy(mirror, me).wait_recv()
    for to in mates + [partner]:
        lcopy(mirror, to).start()

    later = range(1, len(groups))

    @pl.when(is_inner)
    def _():
        for group in later:
            send_layer(group, outer)
        for group in later:
            send_layer(group, sibling)
            send_layer(group, layer, own=True)
            send_layer(group, inner)

    @pl.when(jnp.logical_not(is_inner))
    def _():
        for group in later:
            send_layer(group, outer)
            send_layer(group, inner)
            send_layer(group, sibling)
            send_layer(group, layer, own=True)

    fetch_weight.wait()
    fetch_bias.wait()
    for start in range(0, channels, LANES):
        chosen = swap_matrix(width, width, start, LANES, channels)
        block = jnp.dot(chosen, weight_ref[...], preferred_element_type=jnp.float32)
        wturn[:, start : start + LANES] = block.T.astype(jnp.bfloat16)
    pair = bias_ref.shape[1]
    turned = jnp.broadcast_to(bias_ref[...] * float(seqs), (LANES, pair)).T
    bias_turned[:, :LANES] = turned
    bias_turned[:, LANES:] = turned

    for source in mates:
        for slot in (source, other(source)):
            lcopy(slot, me).wait_recv()
            lcopy(slot, partner).start()
    for source in [me] + mates:
        source = source + 1 - 2 * lax.rem(source, 2)
        for slot in (source, other(source)):
            lcopy(slot, me).wait_recv()
    for s in range(0, n, LANES // TILE):
        block = jnp.concatenate([lbuf[s + p] for p in range(LANES // TILE)], axis=0)
        lturn[:, s * TILE : s * TILE + LANES] = block.T

    def place(chunk, source):
        for p in range(span):
            slot = source * span + p
            start = pl.multiple_of(slot * TILE, TILE)
            block = [rbuf[chunk, slot, :, u * LANES : (u + 1) * LANES] for u in range(turns)]
            for e, wide in enumerate(unpack_columns(cols, period, block)):
                rwide[pl.ds(start, TILE), e * LANES : (e + 1) * LANES] = wide

    def multiply(step):
        lanes = slice(step * 2 * LANES, (step + 1) * 2 * LANES)
        product = jnp.dot(
            lturn[...], rwide[:, lanes], preferred_element_type=jnp.float32
        ).astype(jnp.bfloat16)
        for side_e in range(2):
            at = (step * 2 + side_e) * width
            for i in range(rows):
                side = (i % 2) * LANES
                flat[i // 2, at : at + width, side : side + LANES] = product[
                    i * width : (i + 1) * width, side_e * LANES : (side_e + 1) * LANES
                ]

    def project(chunk, step):
        update = jnp.dot(
            wturn[:, chunk * deep : (chunk + 1) * deep], flat[step],
            preferred_element_type=jnp.float32,
        )
        update = update + (partial[step] if chunk else bias_turned[...])
        if chunk < chunks - 1:
            partial[step] = update
            return
        update = (update * (1.0 / seqs)).astype(out_ref.dtype)
        for side in range(2):
            block = update[:, side * LANES : (side + 1) * LANES].T
            out_ref[2 * step + side] = block[:cols]

    own.wait()
    for group, (first, count) in enumerate(groups):
        arrival(group, layer, span - 1).wait_recv()
        place(first, layer)
        for source in (sibling, outer, inner):
            arrival(group, source, span).wait_recv()
            place(first, source)
        for chunk in range(first, first + count):
            if chunk > first:
                for source in range(LAYERS):
                    place(chunk, source)
            for step in range(period // 2):
                multiply(step)
            for step in range(rows // 2):
                project(chunk, step)

    pltpu.make_async_remote_copy(
        src_ref=sbuf.at[:, pl.ds(0, n - 1)],
        dst_ref=rbuf.at[:, pl.ds(0, n - 1)],
        send_sem=rsend,
        recv_sem=rrecv.at[0, 0],
        device_id={"col": mirror},
        device_id_type=MESH,
    ).wait_send()
    pltpu.make_async_remote_copy(
        src_ref=lbuf.at[pl.ds(0, n - 1)],
        dst_ref=lbuf.at[pl.ds(0, n - 1)],
        send_sem=lsend,
        recv_sem=lrecv.at[0],
        device_id={"col": mirror},
        device_id_type=MESH,
    ).wait_send()


def packed_call(n, left, right, out_weight, out_bias):
    local, rows, width = left.shape
    cols = right.shape[1] // n
    pair = out_weight.shape[1]
    seqs = local * n
    period = LANES // math.gcd(cols, LANES)
    chunks = width // period
    lanes = cols * period
    hbm = pl.BlockSpec(memory_space=pltpu.HBM)
    vmem = pl.BlockSpec(memory_space=pltpu.VMEM)
    dma, regular = pltpu.SemaphoreType.DMA, pltpu.SemaphoreType.REGULAR
    bf16, f32 = jnp.bfloat16, jnp.float32
    return pl.pallas_call(
        functools.partial(packed_kernel, n, cols, period),
        out_shape=jax.ShapeDtypeStruct((rows, cols, pair), bf16),
        in_specs=[hbm] * 4,
        out_specs=vmem,
        scratch_shapes=[
            pltpu.VMEM((local, rows, width), bf16),
            pltpu.VMEM((local, width, n * cols), bf16),
            pltpu.VMEM((width * width, pair), bf16),
            pltpu.VMEM((1, pair), f32),
            pltpu.VMEM((pair, 2 * LANES), f32),
            pltpu.VMEM((local * rows, LANES), f32),
            pltpu.VMEM((n * cols // LANES, local * TILE, LANES), f32),
            pltpu.VMEM((chunks, n, local, lanes), bf16),
            pltpu.VMEM((chunks, n, local, lanes), bf16),
            pltpu.VMEM((n, local, rows * width), bf16),
            pltpu.VMEM((seqs, period * LANES), bf16),
            pltpu.VMEM((rows * width, seqs), bf16),
            pltpu.VMEM((pair, width * width), bf16),
            pltpu.VMEM((rows // 2, period * width, 2 * LANES), bf16),
            pltpu.VMEM((rows // 2, pair, 2 * LANES), f32),
            dma(()), dma((1 + chunks - chunks * TILE // width, LAYERS)), dma(()), dma((n,)),
            dma((3 + width // TILE,)), regular, regular, regular, regular,
        ],
        compiler_params=pltpu.CompilerParams(
            collective_id=0, has_side_effects=True, vmem_limit_bytes=40 * 1024 * 1024
        ),
    )(*(pltpu.with_memory_space_constraint(x, pltpu.HBM) for x in (left, jnp.transpose(right, (0, 2, 1)), out_weight, out_bias.reshape(1, pair))))


def packs(n, left, right):
    local, rows, width = left.shape
    cols = right.shape[1] // n
    period = LANES // math.gcd(cols, LANES)
    return (
        local == TILE and cols <= LANES and rows % 4 == 0 and rows <= 32
        and LANES % width == 0 and rows % (LANES // width) == 0
        and width % TILE == 0 and TILE % period == 0 and period % 2 == 0
        and n % period == 0 and n % (LANES // TILE) == 0 and n % (2 * LAYERS) == 0
        and width // period % (width // TILE) == 0 and n // period % 2 == 0
    )


def flip(x_ref, o_ref, h):
    chunks, columns, lanes = o_ref.shape
    part = x_ref.shape[1] // chunks
    step = 2 * LANES
    for start in range(0, columns, step):
        piece = x_ref[:, h * part : (h + 1) * part, start : start + step]
        o_ref[h, start : start + step] = piece.reshape(lanes, step).T


def swap_matrix(first, minor, start, rows, columns):
    row = lax.broadcasted_iota(jnp.int32, (rows, columns), 0) + start
    column = lax.broadcasted_iota(jnp.int32, (rows, columns), 1)
    shift = first.bit_length() - 1
    wanted = (row & (first - 1)) * minor + (row >> shift)
    return jnp.where(column == wanted, 1.0, 0.0).astype(jnp.bfloat16)


def kernel(
    n, width, cols, rows, chunks, given_ref, left_ref, weight_ref, bias_ref, out_ref,
    right_ref, rbuf, lbuf, rwide, lturn, wturn, flat, partial,
    rsend, rrecv, lsend, lrecv, fsend, own,
):
    me = lax.axis_index("col")
    place = lax.rem(me, GROUP)
    mates = [me - place + lax.rem(place + j, GROUP) for j in range(1, GROUP)]
    hops = n // GROUP
    local = left_ref.shape[0]
    seqs = n * local
    part = width // chunks

    def rcopy(h, k):
        to = lax.rem(me + k, n)
        start = pl.multiple_of(to * cols, TILE)
        return pltpu.make_async_remote_copy(
            src_ref=right_ref.at[h, pl.ds(start, cols)],
            dst_ref=rbuf.at[h, me],
            send_sem=rsend.at[h, k],
            recv_sem=rrecv.at[h, me],
            device_id={"col": to},
            device_id_type=MESH,
        )

    def lcopy(src, slot, to, send):
        return pltpu.make_async_remote_copy(
            src_ref=src,
            dst_ref=lbuf.at[slot],
            send_sem=send,
            recv_sem=lrecv.at[slot],
            device_id={"col": to},
            device_id_type=MESH,
        )

    barrier = pltpu.get_barrier_semaphore()
    for k in range(1, n):
        pl.semaphore_signal(
            barrier, inc=1, device_id={"col": lax.rem(me + k, n)}, device_id_type=MESH
        )
    flip(given_ref, right_ref, 0)
    pl.semaphore_wait(barrier, n - 1)

    sends = []
    for k in range(1, hops):
        sends.append(lcopy(left_ref, me, lax.rem(me + GROUP * k, n), lsend.at[k]))
    for j, mate in enumerate(mates):
        sends.append(lcopy(left_ref, me, mate, fsend.at[0, j]))
    for k in range(1, n):
        sends.append(rcopy(0, k))
    for copy in sends:
        copy.start()
    for h in range(1, chunks):
        flip(given_ref, right_ref, h)
    mine_left = pltpu.make_async_copy(left_ref, lbuf.at[me], own.at[chunks])
    mine_left.start()

    rwide[...] = jnp.zeros_like(rwide)
    channels = width * width
    for start in range(0, channels, LANES):
        chosen = swap_matrix(width, width, start, LANES, channels)
        block = jnp.dot(chosen, weight_ref[...], preferred_element_type=jnp.float32)
        wturn[:, start : start + LANES] = block.T.astype(jnp.bfloat16)
    for h in range(1, chunks):
        later = [rcopy(h, k) for k in range(1, n)]
        for copy in later:
            copy.start()
        sends += later
    mine = []
    for h in range(chunks):
        block = right_ref.at[h, pl.ds(pl.multiple_of(me * cols, TILE), cols)]
        mine.append(pltpu.make_async_copy(block, rbuf.at[h, me], own.at[h]))
        mine[h].start()
    swap = swap_matrix(TILE, part, 0, TILE * part, TILE * part)

    forwards = []
    for k in range(1, hops):
        slot = lax.rem(me + n - GROUP * k, n)
        lcopy(left_ref, slot, mates[0], lsend.at[k]).wait_recv()
        for j, mate in enumerate(mates):
            forward = lcopy(lbuf.at[slot], slot, mate, fsend.at[k, j])
            forward.start()
            forwards.append(forward)
    for k in range(hops):
        for j, mate in enumerate(mates):
            slot = lax.rem(mate + n - GROUP * k, n)
            lcopy(left_ref, slot, mate, fsend.at[k, j]).wait_recv()
    mine_left.wait()
    per = TILE // local
    blocks = []
    for group in range(seqs // TILE):
        parts = [lbuf[group * per + p] for p in range(per)]
        if per > 1:
            parts = [piece.astype(jnp.float32) for piece in parts]
            blocks.append(jnp.concatenate(parts, axis=0).astype(jnp.bfloat16))
        else:
            blocks.append(parts[0])
    lturn[...] = jnp.concatenate(blocks, axis=0).T

    def turn(h, start, block):
        turned = lax.dot_general(
            swap, block, (((1,), (1,)), ((), ())), preferred_element_type=jnp.float32
        ).astype(jnp.bfloat16)
        for e in range(part):
            at = (h * part + e) * LANES
            rwide[pl.ds(start, TILE), at : at + cols] = turned[e * TILE : (e + 1) * TILE]

    def arrive(h):
        def one(k, carry):
            slot = lax.rem(me + n - k, n)
            pltpu.make_async_remote_copy(
                src_ref=right_ref.at[h, pl.ds(0, cols)],
                dst_ref=rbuf.at[h, slot],
                send_sem=rsend.at[h, k],
                recv_sem=rrecv.at[h, slot],
                device_id={"col": slot},
                device_id_type=MESH,
            ).wait_recv()
            if per == 1:
                turn(h, pl.multiple_of(slot * TILE, TILE), rbuf[h, slot])
            return carry

        mine[h].wait()
        if per == 1:
            turn(h, pl.multiple_of(me * TILE, TILE), rbuf[h, me])
        lax.fori_loop(1, n, one, 0)
        if per > 1:
            for group in range(seqs // TILE):
                parts = [rbuf[h, group * per + p] for p in range(per)]
                turn(h, group * TILE, jnp.concatenate(parts, axis=1))

    count = flat.shape[0] * 2

    def multiply(base, h):
        def outer(step, carry):
            lanes = pl.ds(pl.multiple_of(step * 2 * LANES, 2 * LANES), 2 * LANES)
            product = jnp.dot(
                lturn[base * width : (base + count) * width, :],
                rwide[:, lanes],
                preferred_element_type=jnp.float32,
            ).astype(jnp.bfloat16)
            for side_e in range(2):
                at = pl.ds(pl.multiple_of((step * 2 + side_e) * width, width), width)
                for i in range(count):
                    side = (i % 2) * LANES
                    flat[i // 2, at, side : side + LANES] = product[
                        i * width : (i + 1) * width, side_e * LANES : (side_e + 1) * LANES
                    ]
            return carry

        lax.fori_loop(h * part // 2, (h + 1) * part // 2, outer, 0)

    deep = part * width
    early = rows == count and chunks > 1

    def project_early(step, carry):
        partial[step] = jnp.dot(
            wturn[:, : channels - deep],
            flat[step, : channels - deep],
            preferred_element_type=jnp.float32,
        )
        return carry

    for h in range(chunks):
        arrive(h)
        if rows == count:
            multiply(0, h)
        if early and h == chunks - 2:
            lax.fori_loop(0, count // 2, project_early, 0)

    skip = channels - deep if early else 0
    for base in range(0, rows, count):
        if rows != count:
            for h in range(chunks):
                multiply(base, h)

        def project(step, carry):
            update = jnp.dot(
                wturn[:, skip:], flat[step, skip:], preferred_element_type=jnp.float32
            )
            if early:
                update = update + partial[step]
            update = update.T * (1.0 / seqs) + bias_ref[...]
            update = update.astype(out_ref.dtype)
            out_ref[base + 2 * step] = update[:cols]
            out_ref[base + 2 * step + 1] = update[LANES : LANES + cols]
            return carry

        lax.fori_loop(0, count // 2, project, 0)

    for copy in sends + forwards:
        copy.wait_send()


def on_device(n, left, right, out_weight, out_bias):
    if packs(n, left, right):
        return packed_call(n, left, right, out_weight, out_bias)
    local, rows, width = left.shape
    cols = right.shape[1] // n
    pair = out_weight.shape[1]
    seqs = local * n
    chunks = 2 if local * width % (4 * LANES) == 0 else 1
    rows_step = min(rows, 32)
    vmem = pl.BlockSpec(memory_space=pltpu.VMEM)
    dma = pltpu.SemaphoreType.DMA
    return pl.pallas_call(
        functools.partial(kernel, n, width, cols, rows, chunks),
        out_shape=jax.ShapeDtypeStruct((rows, cols, pair), jnp.bfloat16),
        in_specs=[vmem] * 4,
        out_specs=vmem,
        scratch_shapes=[
            pltpu.VMEM((chunks, right.shape[1], local * width // chunks), jnp.bfloat16),
            pltpu.VMEM((chunks, n, cols, local * width // chunks), jnp.bfloat16),
            pltpu.VMEM((n, local, rows * width), jnp.bfloat16),
            pltpu.VMEM((seqs, width * LANES), jnp.bfloat16),
            pltpu.VMEM((rows * width, seqs), jnp.bfloat16),
            pltpu.VMEM((pair, width * width), jnp.bfloat16),
            pltpu.VMEM((rows_step // 2, width * width, 2 * LANES), jnp.bfloat16),
            pltpu.VMEM((rows_step // 2, pair, 2 * LANES), jnp.float32),
            dma((chunks, n)), dma((chunks, n)),
            dma((n // GROUP,)), dma((n,)), dma((n // GROUP, GROUP)), dma((chunks + 1,)),
        ],
        compiler_params=pltpu.CompilerParams(
            collective_id=0, has_side_effects=True, vmem_limit_bytes=40 * 1024 * 1024
        ),
    )(jnp.transpose(right, (0, 2, 1)), left.reshape(local, rows * width), out_weight, out_bias.reshape(1, pair))


def solution(mesh):
    return jax.shard_map(
        functools.partial(on_device, mesh.shape["col"]),
        mesh=mesh,
        in_specs=(P("col", "groups", None), P("col", "groups", None), P(), P()),
        out_specs=P("groups", "col", None),
        check_vma=False,
    )
```

```python
import functools
import math

import jax
import jax.numpy as jnp
from jax import lax
from jax.experimental import pallas as pl
from jax.experimental.pallas import tpu as pltpu
from jax.sharding import PartitionSpec as P

MESH = pl.DeviceIdType.MESH
LANES = 128
TILE = 16
GROUP = 4
LAYERS = 4


def lane_index():
    return lax.broadcasted_iota(jnp.int32, (TILE, LANES), 1)


def turn_lanes(x, shift):
    shift %= LANES
    return pltpu.roll(x, shift, axis=1) if shift else x


def pick(lane, start, left, right):
    return jnp.where(lane >= start, right, left)


def pack_columns(cols, period, tiles):
    lane = lane_index()
    packed = []
    for d in range(period):
        first, offset = divmod(cols * d, LANES)
        moved = []
        for e in range(period):
            piece = tiles[e][first]
            if offset + cols > LANES:
                piece = pick(lane, offset, tiles[e][first + 1], piece)
            moved.append(turn_lanes(piece, cols * e - offset))
        outs = []
        for u in range(cols * period // LANES):
            low, high = u * LANES, (u + 1) * LANES
            out = None
            for e in range(period):
                start = cols * e
                if start + cols <= low or start >= high:
                    continue
                out = moved[e] if out is None else pick(lane, start - low, out, moved[e])
            outs.append(out)
        packed.append(outs)
    return packed


def unpack_columns(cols, period, tiles):
    lane = lane_index()
    wide = []
    for e in range(period):
        first, offset = divmod(cols * e, LANES)
        piece = tiles[first]
        if offset + cols > LANES:
            piece = pick(lane, offset, tiles[first + 1], piece)
        wide.append(turn_lanes(piece, -offset))
    return wide


def packed_kernel(
    n, cols, period, left_hbm, right_hbm, weight_hbm, bias_hbm, out_ref,
    left_ref, right_ref, weight_ref, bias_ref, bias_turned, lspread, rspread, sbuf, rbuf, lbuf,
    rwide, lturn, wturn, flat, partial,
    rsend, rrecv, lsend, lrecv, loads, edges_in, layer_in, far_in, all_in,
):
    me = lax.axis_index("col")
    span = n // LAYERS
    layer, place_in = me // span, lax.rem(me, span)
    sibling = layer + 1 - 2 * lax.rem(layer, 2)
    low = layer < LAYERS // 2
    is_inner = (layer == LAYERS // 2 - 1) | (layer == LAYERS // 2)
    outer = jnp.where(low, LAYERS - 1, 0)
    inner = jnp.where(low, LAYERS // 2, LAYERS // 2 - 1)
    partner = me + 1 - 2 * lax.rem(me, 2)
    near = sibling * span + place_in

    def other(slot):
        return (LAYERS - 1 - slot // span) * span + lax.rem(slot, span)

    mirror = other(me)
    local, rows, width = left_ref.shape
    seqs = n * local
    chunks = width // period
    halves = width // TILE
    per_half = chunks // halves
    channels = width * width
    deep = period * width
    groups = [(0, per_half)] + [(chunk, 1) for chunk in range(per_half, chunks)]
    rest = len(groups)
    groups.append((per_half, chunks - per_half))

    barrier = pltpu.get_barrier_semaphore()

    def greet(semaphore, to):
        pl.semaphore_signal(semaphore, inc=1, device_id={"col": to}, device_id_type=MESH)

    @pl.when(is_inner)
    def _():
        for p in range(span):
            greet(barrier, inner * span + p)
        for p in range(span):
            greet(barrier, sibling * span + p)

    fetch_left = pltpu.make_async_copy(left_hbm, left_ref, loads.at[0])
    fetch_weight = pltpu.make_async_copy(weight_hbm, weight_ref, loads.at[1])
    fetch_bias = pltpu.make_async_copy(bias_hbm, bias_ref, loads.at[2])
    fetch_right = [
        pltpu.make_async_copy(
            right_hbm.at[:, pl.ds(h * TILE, TILE)],
            right_ref.at[:, pl.ds(h * TILE, TILE)],
            loads.at[3 + h],
        )
        for h in range(halves)
    ]
    for fetch in fetch_right:
        fetch.start()
    fetch_left.start()
    fetch_weight.start()
    fetch_bias.start()

    turns = cols * period // LANES
    cycles = n // period

    def spread_half(h):
        fetch_right[h].wait()
        for s in range(local):
            for t in range(turns * cycles):
                rspread[t, s * TILE : (s + 1) * TILE] = right_ref[
                    s, h * TILE : (h + 1) * TILE, t * LANES : (t + 1) * LANES
                ].astype(jnp.float32)

    def pack_half(h, first, count):
        def pack(step, carry):
            chunk, cycle = step // count, first + lax.rem(step, count)
            tiles = [
                [
                    rspread[
                        cycle * turns + t,
                        pl.ds(chunk * period + e, local, stride=TILE),
                    ].astype(jnp.bfloat16)
                    for t in range(turns)
                ]
                for e in range(period)
            ]
            for d, outs in enumerate(pack_columns(cols, period, tiles)):
                for u, out in enumerate(outs):
                    sbuf[
                        h * per_half + chunk, cycle * period + d, :,
                        u * LANES : (u + 1) * LANES,
                    ] = out
            return carry

        lax.fori_loop(0, per_half * count, pack, 0)

    def send_right(group, to):
        first, count = groups[group]
        pltpu.make_async_remote_copy(
            src_ref=sbuf.at[pl.ds(first, count), to],
            dst_ref=rbuf.at[pl.ds(first, count), me],
            send_sem=rsend,
            recv_sem=rrecv.at[group, layer],
            device_id={"col": to},
            device_id_type=MESH,
        ).start()

    def send_layer(group, target, own=False):
        for p in range(int(own), span):
            send_right(group, target * span + lax.rem(place_in + p, span))

    def arrival(group, source, number):
        first, count = groups[group]
        slots = pl.ds(source * span, number)
        return pltpu.make_async_remote_copy(
            src_ref=sbuf.at[pl.ds(first, count), slots],
            dst_ref=rbuf.at[pl.ds(first, count), slots],
            send_sem=rsend,
            recv_sem=rrecv.at[group, source],
            device_id={"col": mirror},
            device_id_type=MESH,
        )

    def lcopy(slot, to):
        return pltpu.make_async_remote_copy(
            src_ref=lbuf.at[slot],
            dst_ref=lbuf.at[slot],
            send_sem=lsend,
            recv_sem=lrecv.at[slot],
            device_id={"col": to},
            device_id_type=MESH,
        )

    mates_near = [
        sibling * span + lax.rem(place_in + 2 * j, span) for j in range(span // 2)
    ]
    mates_own = [
        layer * span + lax.rem(place_in + 2 * j, span) for j in range(1, span // 2)
    ]
    mates = mates_near + mates_own

    half_cycles = cycles // 2
    mine = jnp.where(low, 0, half_cycles)
    theirs = half_cycles - mine
    early = jnp.where(is_inner, theirs, mine)
    spread_half(0)
    pack_half(0, early, half_cycles)
    pl.semaphore_wait(barrier, span)

    @pl.when(is_inner)
    def _():
        greet(layer_in, mirror)
        send_layer(0, inner)

    @pl.when(jnp.logical_not(is_inner))
    def _():
        for p in range(span):
            greet(edges_in, sibling * span + p)
        send_layer(0, sibling)

    pack_half(0, half_cycles - early, half_cycles)
    fetch_left.wait()
    for s in range(local):
        lspread[s * rows : (s + 1) * rows, :width] = left_ref[s].astype(jnp.float32)
    lane = lane_index()
    join = LANES // width
    for t in range(rows // join):
        block = lspread[pl.ds(t * join, local, stride=rows), :]
        for k in range(1, join):
            piece = lspread[pl.ds(t * join + k, local, stride=rows), :]
            block = pick(lane, k * width, block, turn_lanes(piece, k * width))
        lbuf[me, :, t * LANES : (t + 1) * LANES] = block.astype(jnp.bfloat16)

    @pl.when(is_inner)
    def _():
        pl.semaphore_wait(edges_in, span)
        pl.semaphore_wait(layer_in, 1)
        greet(far_in, mirror)
        for to in [mirror] + mates + [partner]:
            lcopy(me, to).start()
        send_layer(0, layer, own=True)
        send_layer(0, sibling)
        pl.semaphore_wait(far_in, 1)
        greet(all_in, near)
        send_layer(0, outer)

    @pl.when(jnp.logical_not(is_inner))
    def _():
        pl.semaphore_wait(all_in, 1)
        for to in [mirror] + mates + [partner]:
            lcopy(me, to).start()
        send_layer(0, layer, own=True)
        send_layer(0, inner)
        send_layer(0, outer)

    for h in range(1, halves):
        spread_half(h)
        pack_half(h, 0, cycles)
    own = pltpu.make_async_copy(sbuf.at[:, me], rbuf.at[:, me], loads.at[0])
    own.start()

    lcopy(mirror, me).wait_recv()
    for to in mates + [partner]:
        lcopy(mirror, to).start()

    later = range(1, rest)

    @pl.when(is_inner & low)
    def _():
        for group in later:
            send_layer(group, inner)
            send_layer(group, sibling)
            send_layer(group, layer, own=True)
            send_layer(group, outer)

    def send_part(group, target, part):
        for p in range(span // 2):
            turn = lax.rem(place_in + p, span // 2)
            send_right(group, target * span + part * (span // 2) + turn)

    @pl.when(is_inner & jnp.logical_not(low))
    def _():
        for group in later:
            send_layer(group, sibling)
            send_layer(group, layer, own=True)
        for group in later[:-1]:
            send_layer(group, outer)
        send_part(later[-1], outer, 0)
        for group in later[:-1]:
            send_layer(group, inner)
        send_part(later[-1], outer, 1)
        send_part(later[-1], inner, 0)
        send_part(later[-1], inner, 1)

    @pl.when(jnp.logical_not(is_inner))
    def _():
        send_layer(rest, outer)
        send_layer(rest, inner)
        for group in later:
            send_layer(group, sibling)
            send_layer(group, layer, own=True)

    fetch_weight.wait()
    fetch_bias.wait()
    for start in range(0, channels, LANES):
        chosen = swap_matrix(width, width, start, LANES, channels)
        block = jnp.dot(chosen, weight_ref[...], preferred_element_type=jnp.float32)
        wturn[:, start : start + LANES] = block.T.astype(jnp.bfloat16)
    pair = bias_ref.shape[1]
    turned = jnp.broadcast_to(bias_ref[...] * float(seqs), (LANES, pair)).T
    bias_turned[:, :LANES] = turned
    bias_turned[:, LANES:] = turned

    for source in mates:
        for slot in (source, other(source)):
            lcopy(slot, me).wait_recv()
            lcopy(slot, partner).start()
    for source in [me] + mates:
        source = source + 1 - 2 * lax.rem(source, 2)
        for slot in (source, other(source)):
            lcopy(slot, me).wait_recv()
    for s in range(0, n, LANES // TILE):
        block = jnp.concatenate([lbuf[s + p] for p in range(LANES // TILE)], axis=0)
        lturn[:, s * TILE : s * TILE + LANES] = block.T

    def place(chunk, source):
        for p in range(span):
            slot = source * span + p
            start = pl.multiple_of(slot * TILE, TILE)
            block = [rbuf[chunk, slot, :, u * LANES : (u + 1) * LANES] for u in range(turns)]
            for e, wide in enumerate(unpack_columns(cols, period, block)):
                rwide[pl.ds(start, TILE), e * LANES : (e + 1) * LANES] = wide

    def multiply(step):
        lanes = slice(step * 2 * LANES, (step + 1) * 2 * LANES)
        product = jnp.dot(
            lturn[...], rwide[:, lanes], preferred_element_type=jnp.float32
        ).astype(jnp.bfloat16)
        for side_e in range(2):
            at = (step * 2 + side_e) * width
            for i in range(rows):
                side = (i % 2) * LANES
                flat[i // 2, at : at + width, side : side + LANES] = product[
                    i * width : (i + 1) * width, side_e * LANES : (side_e + 1) * LANES
                ]

    def project(chunk, step):
        update = jnp.dot(
            wturn[:, chunk * deep : (chunk + 1) * deep], flat[step],
            preferred_element_type=jnp.float32,
        )
        update = update + (partial[step] if chunk else bias_turned[...])
        if chunk < chunks - 1:
            partial[step] = update
            return
        update = (update * (1.0 / seqs)).astype(out_ref.dtype)
        for side in range(2):
            block = update[:, side * LANES : (side + 1) * LANES].T
            out_ref[2 * step + side] = block[:cols]

    own.wait()
    for group, (first, count) in enumerate(groups[:rest]):
        arrival(group, layer, span - 1).wait_recv()
        place(first, layer)
        arrival(group, sibling, span).wait_recv()
        place(first, sibling)
        if group < 2:
            arrival(rest if group else group, outer, span).wait_recv()
        place(first, outer)
        arrival(group, inner, span).wait_recv()
        place(first, inner)
        for chunk in range(first, first + count):
            if chunk > first:
                for source in range(LAYERS):
                    place(chunk, source)
            for step in range(period // 2):
                multiply(step)
            for step in range(rows // 2):
                project(chunk, step)

    pltpu.make_async_remote_copy(
        src_ref=sbuf.at[:, pl.ds(0, n - 1)],
        dst_ref=rbuf.at[:, pl.ds(0, n - 1)],
        send_sem=rsend,
        recv_sem=rrecv.at[0, 0],
        device_id={"col": mirror},
        device_id_type=MESH,
    ).wait_send()
    pltpu.make_async_remote_copy(
        src_ref=lbuf.at[pl.ds(0, n - 1)],
        dst_ref=lbuf.at[pl.ds(0, n - 1)],
        send_sem=lsend,
        recv_sem=lrecv.at[0],
        device_id={"col": mirror},
        device_id_type=MESH,
    ).wait_send()


def packed_call(n, left, right, out_weight, out_bias):
    local, rows, width = left.shape
    cols = right.shape[1] // n
    pair = out_weight.shape[1]
    seqs = local * n
    period = LANES // math.gcd(cols, LANES)
    chunks = width // period
    lanes = cols * period
    hbm = pl.BlockSpec(memory_space=pltpu.HBM)
    vmem = pl.BlockSpec(memory_space=pltpu.VMEM)
    dma, regular = pltpu.SemaphoreType.DMA, pltpu.SemaphoreType.REGULAR
    bf16, f32 = jnp.bfloat16, jnp.float32
    return pl.pallas_call(
        functools.partial(packed_kernel, n, cols, period),
        out_shape=jax.ShapeDtypeStruct((rows, cols, pair), bf16),
        in_specs=[hbm] * 4,
        out_specs=vmem,
        scratch_shapes=[
            pltpu.VMEM((local, rows, width), bf16),
            pltpu.VMEM((local, width, n * cols), bf16),
            pltpu.VMEM((width * width, pair), bf16),
            pltpu.VMEM((1, pair), f32),
            pltpu.VMEM((pair, 2 * LANES), f32),
            pltpu.VMEM((local * rows, LANES), f32),
            pltpu.VMEM((n * cols // LANES, local * TILE, LANES), f32),
            pltpu.VMEM((chunks, n, local, lanes), bf16),
            pltpu.VMEM((chunks, n, local, lanes), bf16),
            pltpu.VMEM((n, local, rows * width), bf16),
            pltpu.VMEM((seqs, period * LANES), bf16),
            pltpu.VMEM((rows * width, seqs), bf16),
            pltpu.VMEM((pair, width * width), bf16),
            pltpu.VMEM((rows // 2, period * width, 2 * LANES), bf16),
            pltpu.VMEM((rows // 2, pair, 2 * LANES), f32),
            dma(()), dma((2 + chunks - chunks * TILE // width, LAYERS)), dma(()), dma((n,)),
            dma((3 + width // TILE,)), regular, regular, regular, regular,
        ],
        compiler_params=pltpu.CompilerParams(
            collective_id=0, has_side_effects=True, vmem_limit_bytes=40 * 1024 * 1024
        ),
    )(*(pltpu.with_memory_space_constraint(x, pltpu.HBM) for x in (left, jnp.transpose(right, (0, 2, 1)), out_weight, out_bias.reshape(1, pair))))


def packs(n, left, right):
    local, rows, width = left.shape
    cols = right.shape[1] // n
    period = LANES // math.gcd(cols, LANES)
    return (
        local == TILE and cols <= LANES and rows % 4 == 0 and rows <= 32
        and LANES % width == 0 and rows % (LANES // width) == 0
        and width % TILE == 0 and TILE % period == 0 and period % 2 == 0
        and n % period == 0 and n % (LANES // TILE) == 0 and n % (2 * LAYERS) == 0
        and width // period % (width // TILE) == 0 and n // period % 2 == 0
    )


def flip(x_ref, o_ref, h):
    chunks, columns, lanes = o_ref.shape
    part = x_ref.shape[1] // chunks
    step = 2 * LANES
    for start in range(0, columns, step):
        piece = x_ref[:, h * part : (h + 1) * part, start : start + step]
        o_ref[h, start : start + step] = piece.reshape(lanes, step).T


def swap_matrix(first, minor, start, rows, columns):
    row = lax.broadcasted_iota(jnp.int32, (rows, columns), 0) + start
    column = lax.broadcasted_iota(jnp.int32, (rows, columns), 1)
    shift = first.bit_length() - 1
    wanted = (row & (first - 1)) * minor + (row >> shift)
    return jnp.where(column == wanted, 1.0, 0.0).astype(jnp.bfloat16)


def kernel(
    n, width, cols, rows, chunks, given_ref, left_ref, weight_ref, bias_ref, out_ref,
    right_ref, rbuf, lbuf, rwide, lturn, wturn, flat, partial,
    rsend, rrecv, lsend, lrecv, fsend, own,
):
    me = lax.axis_index("col")
    place = lax.rem(me, GROUP)
    mates = [me - place + lax.rem(place + j, GROUP) for j in range(1, GROUP)]
    hops = n // GROUP
    local = left_ref.shape[0]
    seqs = n * local
    part = width // chunks

    def rcopy(h, k):
        to = lax.rem(me + k, n)
        start = pl.multiple_of(to * cols, TILE)
        return pltpu.make_async_remote_copy(
            src_ref=right_ref.at[h, pl.ds(start, cols)],
            dst_ref=rbuf.at[h, me],
            send_sem=rsend.at[h, k],
            recv_sem=rrecv.at[h, me],
            device_id={"col": to},
            device_id_type=MESH,
        )

    def lcopy(src, slot, to, send):
        return pltpu.make_async_remote_copy(
            src_ref=src,
            dst_ref=lbuf.at[slot],
            send_sem=send,
            recv_sem=lrecv.at[slot],
            device_id={"col": to},
            device_id_type=MESH,
        )

    barrier = pltpu.get_barrier_semaphore()
    for k in range(1, n):
        pl.semaphore_signal(
            barrier, inc=1, device_id={"col": lax.rem(me + k, n)}, device_id_type=MESH
        )
    flip(given_ref, right_ref, 0)
    pl.semaphore_wait(barrier, n - 1)

    sends = []
    for k in range(1, hops):
        sends.append(lcopy(left_ref, me, lax.rem(me + GROUP * k, n), lsend.at[k]))
    for j, mate in enumerate(mates):
        sends.append(lcopy(left_ref, me, mate, fsend.at[0, j]))
    for k in range(1, n):
        sends.append(rcopy(0, k))
    for copy in sends:
        copy.start()
    for h in range(1, chunks):
        flip(given_ref, right_ref, h)
    mine_left = pltpu.make_async_copy(left_ref, lbuf.at[me], own.at[chunks])
    mine_left.start()

    rwide[...] = jnp.zeros_like(rwide)
    channels = width * width
    for start in range(0, channels, LANES):
        chosen = swap_matrix(width, width, start, LANES, channels)
        block = jnp.dot(chosen, weight_ref[...], preferred_element_type=jnp.float32)
        wturn[:, start : start + LANES] = block.T.astype(jnp.bfloat16)
    for h in range(1, chunks):
        later = [rcopy(h, k) for k in range(1, n)]
        for copy in later:
            copy.start()
        sends += later
    mine = []
    for h in range(chunks):
        block = right_ref.at[h, pl.ds(pl.multiple_of(me * cols, TILE), cols)]
        mine.append(pltpu.make_async_copy(block, rbuf.at[h, me], own.at[h]))
        mine[h].start()
    swap = swap_matrix(TILE, part, 0, TILE * part, TILE * part)

    forwards = []
    for k in range(1, hops):
        slot = lax.rem(me + n - GROUP * k, n)
        lcopy(left_ref, slot, mates[0], lsend.at[k]).wait_recv()
        for j, mate in enumerate(mates):
            forward = lcopy(lbuf.at[slot], slot, mate, fsend.at[k, j])
            forward.start()
            forwards.append(forward)
    for k in range(hops):
        for j, mate in enumerate(mates):
            slot = lax.rem(mate + n - GROUP * k, n)
            lcopy(left_ref, slot, mate, fsend.at[k, j]).wait_recv()
    mine_left.wait()
    per = TILE // local
    blocks = []
    for group in range(seqs // TILE):
        parts = [lbuf[group * per + p] for p in range(per)]
        if per > 1:
            parts = [piece.astype(jnp.float32) for piece in parts]
            blocks.append(jnp.concatenate(parts, axis=0).astype(jnp.bfloat16))
        else:
            blocks.append(parts[0])
    lturn[...] = jnp.concatenate(blocks, axis=0).T

    def turn(h, start, block):
        turned = lax.dot_general(
            swap, block, (((1,), (1,)), ((), ())), preferred_element_type=jnp.float32
        ).astype(jnp.bfloat16)
        for e in range(part):
            at = (h * part + e) * LANES
            rwide[pl.ds(start, TILE), at : at + cols] = turned[e * TILE : (e + 1) * TILE]

    def arrive(h):
        def one(k, carry):
            slot = lax.rem(me + n - k, n)
            pltpu.make_async_remote_copy(
                src_ref=right_ref.at[h, pl.ds(0, cols)],
                dst_ref=rbuf.at[h, slot],
                send_sem=rsend.at[h, k],
                recv_sem=rrecv.at[h, slot],
                device_id={"col": slot},
                device_id_type=MESH,
            ).wait_recv()
            if per == 1:
                turn(h, pl.multiple_of(slot * TILE, TILE), rbuf[h, slot])
            return carry

        mine[h].wait()
        if per == 1:
            turn(h, pl.multiple_of(me * TILE, TILE), rbuf[h, me])
        lax.fori_loop(1, n, one, 0)
        if per > 1:
            for group in range(seqs // TILE):
                parts = [rbuf[h, group * per + p] for p in range(per)]
                turn(h, group * TILE, jnp.concatenate(parts, axis=1))

    count = flat.shape[0] * 2

    def multiply(base, h):
        def outer(step, carry):
            lanes = pl.ds(pl.multiple_of(step * 2 * LANES, 2 * LANES), 2 * LANES)
            product = jnp.dot(
                lturn[base * width : (base + count) * width, :],
                rwide[:, lanes],
                preferred_element_type=jnp.float32,
            ).astype(jnp.bfloat16)
            for side_e in range(2):
                at = pl.ds(pl.multiple_of((step * 2 + side_e) * width, width), width)
                for i in range(count):
                    side = (i % 2) * LANES
                    flat[i // 2, at, side : side + LANES] = product[
                        i * width : (i + 1) * width, side_e * LANES : (side_e + 1) * LANES
                    ]
            return carry

        lax.fori_loop(h * part // 2, (h + 1) * part // 2, outer, 0)

    deep = part * width
    early = rows == count and chunks > 1

    def project_early(step, carry):
        partial[step] = jnp.dot(
            wturn[:, : channels - deep],
            flat[step, : channels - deep],
            preferred_element_type=jnp.float32,
        )
        return carry

    for h in range(chunks):
        arrive(h)
        if rows == count:
            multiply(0, h)
        if early and h == chunks - 2:
            lax.fori_loop(0, count // 2, project_early, 0)

    skip = channels - deep if early else 0
    for base in range(0, rows, count):
        if rows != count:
            for h in range(chunks):
                multiply(base, h)

        def project(step, carry):
            update = jnp.dot(
                wturn[:, skip:], flat[step, skip:], preferred_element_type=jnp.float32
            )
            if early:
                update = update + partial[step]
            update = update.T * (1.0 / seqs) + bias_ref[...]
            update = update.astype(out_ref.dtype)
            out_ref[base + 2 * step] = update[:cols]
            out_ref[base + 2 * step + 1] = update[LANES : LANES + cols]
            return carry

        lax.fori_loop(0, count // 2, project, 0)

    for copy in sends + forwards:
        copy.wait_send()


def on_device(n, left, right, out_weight, out_bias):
    if packs(n, left, right):
        return packed_call(n, left, right, out_weight, out_bias)
    local, rows, width = left.shape
    cols = right.shape[1] // n
    pair = out_weight.shape[1]
    seqs = local * n
    chunks = 2 if local * width % (4 * LANES) == 0 else 1
    rows_step = min(rows, 32)
    vmem = pl.BlockSpec(memory_space=pltpu.VMEM)
    dma = pltpu.SemaphoreType.DMA
    return pl.pallas_call(
        functools.partial(kernel, n, width, cols, rows, chunks),
        out_shape=jax.ShapeDtypeStruct((rows, cols, pair), jnp.bfloat16),
        in_specs=[vmem] * 4,
        out_specs=vmem,
        scratch_shapes=[
            pltpu.VMEM((chunks, right.shape[1], local * width // chunks), jnp.bfloat16),
            pltpu.VMEM((chunks, n, cols, local * width // chunks), jnp.bfloat16),
            pltpu.VMEM((n, local, rows * width), jnp.bfloat16),
            pltpu.VMEM((seqs, width * LANES), jnp.bfloat16),
            pltpu.VMEM((rows * width, seqs), jnp.bfloat16),
            pltpu.VMEM((pair, width * width), jnp.bfloat16),
            pltpu.VMEM((rows_step // 2, width * width, 2 * LANES), jnp.bfloat16),
            pltpu.VMEM((rows_step // 2, pair, 2 * LANES), jnp.float32),
            dma((chunks, n)), dma((chunks, n)),
            dma((n // GROUP,)), dma((n,)), dma((n // GROUP, GROUP)), dma((chunks + 1,)),
        ],
        compiler_params=pltpu.CompilerParams(
            collective_id=0, has_side_effects=True, vmem_limit_bytes=40 * 1024 * 1024
        ),
    )(jnp.transpose(right, (0, 2, 1)), left.reshape(local, rows * width), out_weight, out_bias.reshape(1, pair))


def solution(mesh):
    return jax.shard_map(
        functools.partial(on_device, mesh.shape["col"]),
        mesh=mesh,
        in_specs=(P("col", "groups", None), P("col", "groups", None), P(), P()),
        out_specs=P("groups", "col", None),
        check_vma=False,
    )
```

```python
import functools
import math

import jax
import jax.numpy as jnp
from jax import lax
from jax.experimental import pallas as pl
from jax.experimental.pallas import tpu as pltpu
from jax.sharding import PartitionSpec as P

MESH = pl.DeviceIdType.MESH
LANES = 128
TILE = 16
GROUP = 4
LAYERS = 4


def lane_index():
    return lax.broadcasted_iota(jnp.int32, (TILE, LANES), 1)


def turn_lanes(x, shift):
    shift %= LANES
    return pltpu.roll(x, shift, axis=1) if shift else x


def pick(lane, start, left, right):
    return jnp.where(lane >= start, right, left)


def pack_columns(cols, period, tiles):
    lane = lane_index()
    packed = []
    for d in range(period):
        first, offset = divmod(cols * d, LANES)
        moved = []
        for e in range(period):
            piece = tiles[e][first]
            if offset + cols > LANES:
                piece = pick(lane, offset, tiles[e][first + 1], piece)
            moved.append(turn_lanes(piece, cols * e - offset))
        outs = []
        for u in range(cols * period // LANES):
            low, high = u * LANES, (u + 1) * LANES
            out = None
            for e in range(period):
                start = cols * e
                if start + cols <= low or start >= high:
                    continue
                out = moved[e] if out is None else pick(lane, start - low, out, moved[e])
            outs.append(out)
        packed.append(outs)
    return packed


def unpack_columns(cols, period, tiles):
    lane = lane_index()
    wide = []
    for e in range(period):
        first, offset = divmod(cols * e, LANES)
        piece = tiles[first]
        if offset + cols > LANES:
            piece = pick(lane, offset, tiles[first + 1], piece)
        wide.append(turn_lanes(piece, -offset))
    return wide


def packed_kernel(
    n, cols, period, left_hbm, right_hbm, weight_hbm, bias_hbm, out_ref,
    left_ref, right_ref, weight_ref, bias_ref, bias_turned, lspread, rspread, sbuf, rbuf, lbuf,
    rwide, lturn, wturn, flat, partial,
    rsend, rrecv, lsend, lrecv, loads, edges_in, layer_in, far_in, all_in,
):
    me = lax.axis_index("col")
    span = n // LAYERS
    layer, place_in = me // span, lax.rem(me, span)
    sibling = layer + 1 - 2 * lax.rem(layer, 2)
    low = layer < LAYERS // 2
    is_inner = (layer == LAYERS // 2 - 1) | (layer == LAYERS // 2)
    outer = jnp.where(low, LAYERS - 1, 0)
    inner = jnp.where(low, LAYERS // 2, LAYERS // 2 - 1)
    partner = me + 1 - 2 * lax.rem(me, 2)
    near = sibling * span + place_in

    def other(slot):
        return (LAYERS - 1 - slot // span) * span + lax.rem(slot, span)

    mirror = other(me)
    local, rows, width = left_ref.shape
    seqs = n * local
    chunks = width // period
    halves = width // TILE
    per_half = chunks // halves
    channels = width * width
    deep = period * width
    groups = [(0, per_half)] + [(chunk, 1) for chunk in range(per_half, chunks)]
    rest = len(groups)
    groups.append((per_half, chunks - per_half))

    barrier = pltpu.get_barrier_semaphore()

    def greet(semaphore, to):
        pl.semaphore_signal(semaphore, inc=1, device_id={"col": to}, device_id_type=MESH)

    @pl.when(is_inner)
    def _():
        for p in range(span):
            greet(barrier, inner * span + p)
        for p in range(span):
            greet(barrier, sibling * span + p)

    fetch_left = pltpu.make_async_copy(left_hbm, left_ref, loads.at[0])
    fetch_weight = pltpu.make_async_copy(weight_hbm, weight_ref, loads.at[1])
    fetch_bias = pltpu.make_async_copy(bias_hbm, bias_ref, loads.at[2])
    fetch_right = [
        pltpu.make_async_copy(
            right_hbm.at[:, pl.ds(h * TILE, TILE)],
            right_ref.at[:, pl.ds(h * TILE, TILE)],
            loads.at[3 + h],
        )
        for h in range(halves)
    ]
    for fetch in fetch_right:
        fetch.start()
    fetch_left.start()
    fetch_weight.start()
    fetch_bias.start()

    turns = cols * period // LANES
    cycles = n // period

    def spread_half(h):
        fetch_right[h].wait()
        for s in range(local):
            for t in range(turns * cycles):
                rspread[t, s * TILE : (s + 1) * TILE] = right_ref[
                    s, h * TILE : (h + 1) * TILE, t * LANES : (t + 1) * LANES
                ].astype(jnp.float32)

    def pack_half(h, first, count):
        def pack(step, carry):
            chunk, cycle = step // count, first + lax.rem(step, count)
            tiles = [
                [
                    rspread[
                        cycle * turns + t,
                        pl.ds(chunk * period + e, local, stride=TILE),
                    ].astype(jnp.bfloat16)
                    for t in range(turns)
                ]
                for e in range(period)
            ]
            for d, outs in enumerate(pack_columns(cols, period, tiles)):
                for u, out in enumerate(outs):
                    sbuf[
                        h * per_half + chunk, cycle * period + d, :,
                        u * LANES : (u + 1) * LANES,
                    ] = out
            return carry

        lax.fori_loop(0, per_half * count, pack, 0)

    def send_right(group, to):
        first, count = groups[group]
        pltpu.make_async_remote_copy(
            src_ref=sbuf.at[pl.ds(first, count), to],
            dst_ref=rbuf.at[pl.ds(first, count), me],
            send_sem=rsend,
            recv_sem=rrecv.at[group, layer],
            device_id={"col": to},
            device_id_type=MESH,
        ).start()

    def send_layer(group, target, own=False):
        for p in range(int(own), span):
            send_right(group, target * span + lax.rem(place_in + p, span))

    def arrival(group, source, number):
        first, count = groups[group]
        slots = pl.ds(source * span, number)
        return pltpu.make_async_remote_copy(
            src_ref=sbuf.at[pl.ds(first, count), slots],
            dst_ref=rbuf.at[pl.ds(first, count), slots],
            send_sem=rsend,
            recv_sem=rrecv.at[group, source],
            device_id={"col": mirror},
            device_id_type=MESH,
        )

    def lcopy(slot, to):
        return pltpu.make_async_remote_copy(
            src_ref=lbuf.at[slot],
            dst_ref=lbuf.at[slot],
            send_sem=lsend,
            recv_sem=lrecv.at[slot],
            device_id={"col": to},
            device_id_type=MESH,
        )

    mates_near = [
        sibling * span + lax.rem(place_in + 2 * j, span) for j in range(span // 2)
    ]
    mates_own = [
        layer * span + lax.rem(place_in + 2 * j, span) for j in range(1, span // 2)
    ]
    mates = mates_near + mates_own

    half_cycles = cycles // 2
    mine = jnp.where(low, 0, half_cycles)
    theirs = half_cycles - mine
    early = jnp.where(is_inner, theirs, mine)
    spread_half(0)
    pack_half(0, early, half_cycles)
    pl.semaphore_wait(barrier, span)

    @pl.when(is_inner)
    def _():
        greet(layer_in, mirror)
        send_layer(0, inner)

    @pl.when(jnp.logical_not(is_inner))
    def _():
        for p in range(span):
            greet(edges_in, sibling * span + p)
        send_layer(0, sibling)

    pack_half(0, half_cycles - early, half_cycles)
    fetch_left.wait()
    for s in range(local):
        lspread[s * rows : (s + 1) * rows, :width] = left_ref[s].astype(jnp.float32)
    lane = lane_index()
    join = LANES // width
    for t in range(rows // join):
        block = lspread[pl.ds(t * join, local, stride=rows), :]
        for k in range(1, join):
            piece = lspread[pl.ds(t * join + k, local, stride=rows), :]
            block = pick(lane, k * width, block, turn_lanes(piece, k * width))
        lbuf[me, :, t * LANES : (t + 1) * LANES] = block.astype(jnp.bfloat16)

    @pl.when(is_inner)
    def _():
        pl.semaphore_wait(edges_in, span)
        pl.semaphore_wait(layer_in, 1)
        greet(far_in, mirror)
        for to in [mirror] + mates + [partner]:
            lcopy(me, to).start()
        send_layer(0, layer, own=True)
        send_layer(0, sibling)
        pl.semaphore_wait(far_in, 1)
        greet(all_in, near)
        send_layer(0, outer)

    @pl.when(jnp.logical_not(is_inner))
    def _():
        pl.semaphore_wait(all_in, 1)
        for to in [mirror] + mates + [partner]:
            lcopy(me, to).start()
        send_layer(0, layer, own=True)
        send_layer(0, inner)
        send_layer(0, outer)

    for h in range(1, halves):
        spread_half(h)
        pack_half(h, 0, cycles)
    own = pltpu.make_async_copy(sbuf.at[:, me], rbuf.at[:, me], loads.at[0])
    own.start()

    lcopy(mirror, me).wait_recv()
    for to in mates + [partner]:
        lcopy(mirror, to).start()

    later = range(1, rest)

    @pl.when(is_inner & low)
    def _():
        for group in later:
            send_layer(group, inner)
            send_layer(group, sibling)
            send_layer(group, layer, own=True)
            send_layer(group, outer)

    def send_part(group, target, part):
        for p in range(span // 2):
            turn = lax.rem(place_in + p, span // 2)
            send_right(group, target * span + part * (span // 2) + turn)

    @pl.when(is_inner & jnp.logical_not(low))
    def _():
        for group in later:
            send_layer(group, sibling)
            send_layer(group, layer, own=True)
        for group in later[:-1]:
            send_layer(group, outer)
        for group in later[:-1]:
            send_part(group, inner, 0)
        send_part(later[-1], outer, 0)
        for group in later[:-1]:
            send_part(group, inner, 1)
        for p in range(1, span // 2):
            send_right(later[-1], inner * span + p)
        send_part(later[-1], outer, 1)
        send_right(later[-1], inner * span)
        send_part(later[-1], inner, 1)

    @pl.when(jnp.logical_not(is_inner))
    def _():
        for group in later:
            send_layer(group, sibling)
            send_layer(group, layer, own=True)
        send_layer(rest, outer)
        send_layer(rest, inner)

    fetch_weight.wait()
    fetch_bias.wait()
    for start in range(0, channels, LANES):
        chosen = swap_matrix(width, width, start, LANES, channels)
        block = jnp.dot(chosen, weight_ref[...], preferred_element_type=jnp.float32)
        wturn[:, start : start + LANES] = block.T.astype(jnp.bfloat16)
    pair = bias_ref.shape[1]
    turned = jnp.broadcast_to(bias_ref[...] * float(seqs), (LANES, pair)).T
    bias_turned[:, :LANES] = turned
    bias_turned[:, LANES:] = turned

    for source in mates:
        for slot in (source, other(source)):
            lcopy(slot, me).wait_recv()
            lcopy(slot, partner).start()
    for source in [me] + mates:
        source = source + 1 - 2 * lax.rem(source, 2)
        for slot in (source, other(source)):
            lcopy(slot, me).wait_recv()
    for s in range(0, n, LANES // TILE):
        block = jnp.concatenate([lbuf[s + p] for p in range(LANES // TILE)], axis=0)
        lturn[:, s * TILE : s * TILE + LANES] = block.T

    def place(chunk, source):
        for p in range(span):
            slot = source * span + p
            start = pl.multiple_of(slot * TILE, TILE)
            block = [rbuf[chunk, slot, :, u * LANES : (u + 1) * LANES] for u in range(turns)]
            for e, wide in enumerate(unpack_columns(cols, period, block)):
                rwide[pl.ds(start, TILE), e * LANES : (e + 1) * LANES] = wide

    def multiply(step):
        lanes = slice(step * 2 * LANES, (step + 1) * 2 * LANES)
        product = jnp.dot(
            lturn[...], rwide[:, lanes], preferred_element_type=jnp.float32
        ).astype(jnp.bfloat16)
        for side_e in range(2):
            at = (step * 2 + side_e) * width
            for i in range(rows):
                side = (i % 2) * LANES
                flat[i // 2, at : at + width, side : side + LANES] = product[
                    i * width : (i + 1) * width, side_e * LANES : (side_e + 1) * LANES
                ]

    def project(chunk, step):
        update = jnp.dot(
            wturn[:, chunk * deep : (chunk + 1) * deep], flat[step],
            preferred_element_type=jnp.float32,
        )
        update = update + (partial[step] if chunk else bias_turned[...])
        if chunk < chunks - 1:
            partial[step] = update
            return
        update = (update * (1.0 / seqs)).astype(out_ref.dtype)
        for side in range(2):
            block = update[:, side * LANES : (side + 1) * LANES].T
            out_ref[2 * step + side] = block[:cols]

    own.wait()
    for group, (first, count) in enumerate(groups[:rest]):
        arrival(group, layer, span - 1).wait_recv()
        place(first, layer)
        arrival(group, sibling, span).wait_recv()
        place(first, sibling)
        if group < 2:
            arrival(rest if group else group, outer, span).wait_recv()
        place(first, outer)
        arrival(group, inner, span).wait_recv()
        place(first, inner)
        for chunk in range(first, first + count):
            if chunk > first:
                for source in range(LAYERS):
                    place(chunk, source)
            for step in range(period // 2):
                multiply(step)
            for step in range(rows // 2):
                project(chunk, step)

    pltpu.make_async_remote_copy(
        src_ref=sbuf.at[:, pl.ds(0, n - 1)],
        dst_ref=rbuf.at[:, pl.ds(0, n - 1)],
        send_sem=rsend,
        recv_sem=rrecv.at[0, 0],
        device_id={"col": mirror},
        device_id_type=MESH,
    ).wait_send()
    pltpu.make_async_remote_copy(
        src_ref=lbuf.at[pl.ds(0, n - 1)],
        dst_ref=lbuf.at[pl.ds(0, n - 1)],
        send_sem=lsend,
        recv_sem=lrecv.at[0],
        device_id={"col": mirror},
        device_id_type=MESH,
    ).wait_send()


def packed_call(n, left, right, out_weight, out_bias):
    local, rows, width = left.shape
    cols = right.shape[1] // n
    pair = out_weight.shape[1]
    seqs = local * n
    period = LANES // math.gcd(cols, LANES)
    chunks = width // period
    lanes = cols * period
    hbm = pl.BlockSpec(memory_space=pltpu.HBM)
    vmem = pl.BlockSpec(memory_space=pltpu.VMEM)
    dma, regular = pltpu.SemaphoreType.DMA, pltpu.SemaphoreType.REGULAR
    bf16, f32 = jnp.bfloat16, jnp.float32
    return pl.pallas_call(
        functools.partial(packed_kernel, n, cols, period),
        out_shape=jax.ShapeDtypeStruct((rows, cols, pair), bf16),
        in_specs=[hbm] * 4,
        out_specs=vmem,
        scratch_shapes=[
            pltpu.VMEM((local, rows, width), bf16),
            pltpu.VMEM((local, width, n * cols), bf16),
            pltpu.VMEM((width * width, pair), bf16),
            pltpu.VMEM((1, pair), f32),
            pltpu.VMEM((pair, 2 * LANES), f32),
            pltpu.VMEM((local * rows, LANES), f32),
            pltpu.VMEM((n * cols // LANES, local * TILE, LANES), f32),
            pltpu.VMEM((chunks, n, local, lanes), bf16),
            pltpu.VMEM((chunks, n, local, lanes), bf16),
            pltpu.VMEM((n, local, rows * width), bf16),
            pltpu.VMEM((seqs, period * LANES), bf16),
            pltpu.VMEM((rows * width, seqs), bf16),
            pltpu.VMEM((pair, width * width), bf16),
            pltpu.VMEM((rows // 2, period * width, 2 * LANES), bf16),
            pltpu.VMEM((rows // 2, pair, 2 * LANES), f32),
            dma(()), dma((2 + chunks - chunks * TILE // width, LAYERS)), dma(()), dma((n,)),
            dma((3 + width // TILE,)), regular, regular, regular, regular,
        ],
        compiler_params=pltpu.CompilerParams(
            collective_id=0, has_side_effects=True, vmem_limit_bytes=40 * 1024 * 1024
        ),
    )(*(pltpu.with_memory_space_constraint(x, pltpu.HBM) for x in (left, jnp.transpose(right, (0, 2, 1)), out_weight, out_bias.reshape(1, pair))))


def packs(n, left, right):
    local, rows, width = left.shape
    cols = right.shape[1] // n
    period = LANES // math.gcd(cols, LANES)
    return (
        local == TILE and cols <= LANES and rows % 4 == 0 and rows <= 32
        and LANES % width == 0 and rows % (LANES // width) == 0
        and width % TILE == 0 and TILE % period == 0 and period % 2 == 0
        and n % period == 0 and n % (LANES // TILE) == 0 and n % (2 * LAYERS) == 0
        and width // period % (width // TILE) == 0 and n // period % 2 == 0
    )


def flip(x_ref, o_ref, h):
    chunks, columns, lanes = o_ref.shape
    part = x_ref.shape[1] // chunks
    step = 2 * LANES
    for start in range(0, columns, step):
        piece = x_ref[:, h * part : (h + 1) * part, start : start + step]
        o_ref[h, start : start + step] = piece.reshape(lanes, step).T


def swap_matrix(first, minor, start, rows, columns):
    row = lax.broadcasted_iota(jnp.int32, (rows, columns), 0) + start
    column = lax.broadcasted_iota(jnp.int32, (rows, columns), 1)
    shift = first.bit_length() - 1
    wanted = (row & (first - 1)) * minor + (row >> shift)
    return jnp.where(column == wanted, 1.0, 0.0).astype(jnp.bfloat16)


def kernel(
    n, width, cols, rows, chunks, given_ref, left_ref, weight_ref, bias_ref, out_ref,
    right_ref, rbuf, lbuf, rwide, lturn, wturn, flat, partial,
    rsend, rrecv, lsend, lrecv, fsend, own,
):
    me = lax.axis_index("col")
    place = lax.rem(me, GROUP)
    mates = [me - place + lax.rem(place + j, GROUP) for j in range(1, GROUP)]
    hops = n // GROUP
    local = left_ref.shape[0]
    seqs = n * local
    part = width // chunks

    def rcopy(h, k):
        to = lax.rem(me + k, n)
        start = pl.multiple_of(to * cols, TILE)
        return pltpu.make_async_remote_copy(
            src_ref=right_ref.at[h, pl.ds(start, cols)],
            dst_ref=rbuf.at[h, me],
            send_sem=rsend.at[h, k],
            recv_sem=rrecv.at[h, me],
            device_id={"col": to},
            device_id_type=MESH,
        )

    def lcopy(src, slot, to, send):
        return pltpu.make_async_remote_copy(
            src_ref=src,
            dst_ref=lbuf.at[slot],
            send_sem=send,
            recv_sem=lrecv.at[slot],
            device_id={"col": to},
            device_id_type=MESH,
        )

    barrier = pltpu.get_barrier_semaphore()
    for k in range(1, n):
        pl.semaphore_signal(
            barrier, inc=1, device_id={"col": lax.rem(me + k, n)}, device_id_type=MESH
        )
    flip(given_ref, right_ref, 0)
    pl.semaphore_wait(barrier, n - 1)

    sends = []
    for k in range(1, hops):
        sends.append(lcopy(left_ref, me, lax.rem(me + GROUP * k, n), lsend.at[k]))
    for j, mate in enumerate(mates):
        sends.append(lcopy(left_ref, me, mate, fsend.at[0, j]))
    for k in range(1, n):
        sends.append(rcopy(0, k))
    for copy in sends:
        copy.start()
    for h in range(1, chunks):
        flip(given_ref, right_ref, h)
    mine_left = pltpu.make_async_copy(left_ref, lbuf.at[me], own.at[chunks])
    mine_left.start()

    rwide[...] = jnp.zeros_like(rwide)
    channels = width * width
    for start in range(0, channels, LANES):
        chosen = swap_matrix(width, width, start, LANES, channels)
        block = jnp.dot(chosen, weight_ref[...], preferred_element_type=jnp.float32)
        wturn[:, start : start + LANES] = block.T.astype(jnp.bfloat16)
    for h in range(1, chunks):
        later = [rcopy(h, k) for k in range(1, n)]
        for copy in later:
            copy.start()
        sends += later
    mine = []
    for h in range(chunks):
        block = right_ref.at[h, pl.ds(pl.multiple_of(me * cols, TILE), cols)]
        mine.append(pltpu.make_async_copy(block, rbuf.at[h, me], own.at[h]))
        mine[h].start()
    swap = swap_matrix(TILE, part, 0, TILE * part, TILE * part)

    forwards = []
    for k in range(1, hops):
        slot = lax.rem(me + n - GROUP * k, n)
        lcopy(left_ref, slot, mates[0], lsend.at[k]).wait_recv()
        for j, mate in enumerate(mates):
            forward = lcopy(lbuf.at[slot], slot, mate, fsend.at[k, j])
            forward.start()
            forwards.append(forward)
    for k in range(hops):
        for j, mate in enumerate(mates):
            slot = lax.rem(mate + n - GROUP * k, n)
            lcopy(left_ref, slot, mate, fsend.at[k, j]).wait_recv()
    mine_left.wait()
    per = TILE // local
    blocks = []
    for group in range(seqs // TILE):
        parts = [lbuf[group * per + p] for p in range(per)]
        if per > 1:
            parts = [piece.astype(jnp.float32) for piece in parts]
            blocks.append(jnp.concatenate(parts, axis=0).astype(jnp.bfloat16))
        else:
            blocks.append(parts[0])
    lturn[...] = jnp.concatenate(blocks, axis=0).T

    def turn(h, start, block):
        turned = lax.dot_general(
            swap, block, (((1,), (1,)), ((), ())), preferred_element_type=jnp.float32
        ).astype(jnp.bfloat16)
        for e in range(part):
            at = (h * part + e) * LANES
            rwide[pl.ds(start, TILE), at : at + cols] = turned[e * TILE : (e + 1) * TILE]

    def arrive(h):
        def one(k, carry):
            slot = lax.rem(me + n - k, n)
            pltpu.make_async_remote_copy(
                src_ref=right_ref.at[h, pl.ds(0, cols)],
                dst_ref=rbuf.at[h, slot],
                send_sem=rsend.at[h, k],
                recv_sem=rrecv.at[h, slot],
                device_id={"col": slot},
                device_id_type=MESH,
            ).wait_recv()
            if per == 1:
                turn(h, pl.multiple_of(slot * TILE, TILE), rbuf[h, slot])
            return carry

        mine[h].wait()
        if per == 1:
            turn(h, pl.multiple_of(me * TILE, TILE), rbuf[h, me])
        lax.fori_loop(1, n, one, 0)
        if per > 1:
            for group in range(seqs // TILE):
                parts = [rbuf[h, group * per + p] for p in range(per)]
                turn(h, group * TILE, jnp.concatenate(parts, axis=1))

    count = flat.shape[0] * 2

    def multiply(base, h):
        def outer(step, carry):
            lanes = pl.ds(pl.multiple_of(step * 2 * LANES, 2 * LANES), 2 * LANES)
            product = jnp.dot(
                lturn[base * width : (base + count) * width, :],
                rwide[:, lanes],
                preferred_element_type=jnp.float32,
            ).astype(jnp.bfloat16)
            for side_e in range(2):
                at = pl.ds(pl.multiple_of((step * 2 + side_e) * width, width), width)
                for i in range(count):
                    side = (i % 2) * LANES
                    flat[i // 2, at, side : side + LANES] = product[
                        i * width : (i + 1) * width, side_e * LANES : (side_e + 1) * LANES
                    ]
            return carry

        lax.fori_loop(h * part // 2, (h + 1) * part // 2, outer, 0)

    deep = part * width
    early = rows == count and chunks > 1

    def project_early(step, carry):
        partial[step] = jnp.dot(
            wturn[:, : channels - deep],
            flat[step, : channels - deep],
            preferred_element_type=jnp.float32,
        )
        return carry

    for h in range(chunks):
        arrive(h)
        if rows == count:
            multiply(0, h)
        if early and h == chunks - 2:
            lax.fori_loop(0, count // 2, project_early, 0)

    skip = channels - deep if early else 0
    for base in range(0, rows, count):
        if rows != count:
            for h in range(chunks):
                multiply(base, h)

        def project(step, carry):
            update = jnp.dot(
                wturn[:, skip:], flat[step, skip:], preferred_element_type=jnp.float32
            )
            if early:
                update = update + partial[step]
            update = update.T * (1.0 / seqs) + bias_ref[...]
            update = update.astype(out_ref.dtype)
            out_ref[base + 2 * step] = update[:cols]
            out_ref[base + 2 * step + 1] = update[LANES : LANES + cols]
            return carry

        lax.fori_loop(0, count // 2, project, 0)

    for copy in sends + forwards:
        copy.wait_send()


def on_device(n, left, right, out_weight, out_bias):
    if packs(n, left, right):
        return packed_call(n, left, right, out_weight, out_bias)
    local, rows, width = left.shape
    cols = right.shape[1] // n
    pair = out_weight.shape[1]
    seqs = local * n
    chunks = 2 if local * width % (4 * LANES) == 0 else 1
    rows_step = min(rows, 32)
    vmem = pl.BlockSpec(memory_space=pltpu.VMEM)
    dma = pltpu.SemaphoreType.DMA
    return pl.pallas_call(
        functools.partial(kernel, n, width, cols, rows, chunks),
        out_shape=jax.ShapeDtypeStruct((rows, cols, pair), jnp.bfloat16),
        in_specs=[vmem] * 4,
        out_specs=vmem,
        scratch_shapes=[
            pltpu.VMEM((chunks, right.shape[1], local * width // chunks), jnp.bfloat16),
            pltpu.VMEM((chunks, n, cols, local * width // chunks), jnp.bfloat16),
            pltpu.VMEM((n, local, rows * width), jnp.bfloat16),
            pltpu.VMEM((seqs, width * LANES), jnp.bfloat16),
            pltpu.VMEM((rows * width, seqs), jnp.bfloat16),
            pltpu.VMEM((pair, width * width), jnp.bfloat16),
            pltpu.VMEM((rows_step // 2, width * width, 2 * LANES), jnp.bfloat16),
            pltpu.VMEM((rows_step // 2, pair, 2 * LANES), jnp.float32),
            dma((chunks, n)), dma((chunks, n)),
            dma((n // GROUP,)), dma((n,)), dma((n // GROUP, GROUP)), dma((chunks + 1,)),
        ],
        compiler_params=pltpu.CompilerParams(
            collective_id=0, has_side_effects=True, vmem_limit_bytes=40 * 1024 * 1024
        ),
    )(jnp.transpose(right, (0, 2, 1)), left.reshape(local, rows * width), out_weight, out_bias.reshape(1, pair))


def solution(mesh):
    return jax.shard_map(
        functools.partial(on_device, mesh.shape["col"]),
        mesh=mesh,
        in_specs=(P("col", "groups", None), P("col", "groups", None), P(), P()),
        out_specs=P("groups", "col", None),
        check_vma=False,
    )
```

```python
import functools
import math

import jax
import jax.numpy as jnp
from jax import lax
from jax.experimental import pallas as pl
from jax.experimental.pallas import tpu as pltpu
from jax.sharding import PartitionSpec as P

MESH = pl.DeviceIdType.MESH
LANES = 128
TILE = 16
GROUP = 4
LAYERS = 4
STORES = 8


def lane_index():
    return lax.broadcasted_iota(jnp.int32, (TILE, LANES), 1)


def turn_lanes(x, shift):
    shift %= LANES
    return pltpu.roll(x, shift, axis=1) if shift else x


def pick(lane, start, left, right):
    return jnp.where(lane >= start, right, left)


def pack_columns(cols, period, tiles):
    lane = lane_index()
    packed = []
    for d in range(period):
        first, offset = divmod(cols * d, LANES)
        moved = []
        for e in range(period):
            piece = tiles[e][first]
            if offset + cols > LANES:
                piece = pick(lane, offset, tiles[e][first + 1], piece)
            moved.append(turn_lanes(piece, cols * e - offset))
        outs = []
        for u in range(cols * period // LANES):
            low, high = u * LANES, (u + 1) * LANES
            out = None
            for e in range(period):
                start = cols * e
                if start + cols <= low or start >= high:
                    continue
                out = moved[e] if out is None else pick(lane, start - low, out, moved[e])
            outs.append(out)
        packed.append(outs)
    return packed


def unpack_columns(cols, period, tiles):
    lane = lane_index()
    wide = []
    for e in range(period):
        first, offset = divmod(cols * e, LANES)
        piece = tiles[first]
        if offset + cols > LANES:
            piece = pick(lane, offset, tiles[first + 1], piece)
        wide.append(turn_lanes(piece, -offset))
    return wide


def packed_kernel(
    n, cols, period, left_hbm, right_hbm, weight_hbm, bias_hbm, flat, partial, last,
    left_ref, right_ref, weight_ref, bias_ref, bias_turned, lspread, rspread, sbuf, rbuf, lbuf,
    rwide, lturn, wturn,
    rsend, rrecv, lsend, lrecv, loads, edges_in, layer_in, far_in, all_in,
):
    me = lax.axis_index("col")
    span = n // LAYERS
    layer, place_in = me // span, lax.rem(me, span)
    sibling = layer + 1 - 2 * lax.rem(layer, 2)
    low = layer < LAYERS // 2
    is_inner = (layer == LAYERS // 2 - 1) | (layer == LAYERS // 2)
    outer = jnp.where(low, LAYERS - 1, 0)
    inner = jnp.where(low, LAYERS // 2, LAYERS // 2 - 1)
    partner = me + 1 - 2 * lax.rem(me, 2)
    near = sibling * span + place_in

    def other(slot):
        return (LAYERS - 1 - slot // span) * span + lax.rem(slot, span)

    mirror = other(me)
    local, rows, width = left_ref.shape
    seqs = n * local
    chunks = width // period
    halves = width // TILE
    per_half = chunks // halves
    channels = width * width
    deep = period * width
    groups = [(0, per_half)] + [(chunk, 1) for chunk in range(per_half, chunks)]
    rest = len(groups)
    groups.append((per_half, chunks - per_half))

    barrier = pltpu.get_barrier_semaphore()

    def greet(semaphore, to):
        pl.semaphore_signal(semaphore, inc=1, device_id={"col": to}, device_id_type=MESH)

    @pl.when(is_inner)
    def _():
        for p in range(span):
            greet(barrier, inner * span + p)
        for p in range(span):
            greet(barrier, sibling * span + p)

    fetch_left = pltpu.make_async_copy(left_hbm, left_ref, loads.at[0])
    fetch_weight = pltpu.make_async_copy(weight_hbm, weight_ref, loads.at[1])
    fetch_bias = pltpu.make_async_copy(bias_hbm, bias_ref, loads.at[2])
    fetch_right = [
        pltpu.make_async_copy(
            right_hbm.at[:, pl.ds(h * TILE, TILE)],
            right_ref.at[:, pl.ds(h * TILE, TILE)],
            loads.at[3 + h],
        )
        for h in range(halves)
    ]
    for fetch in fetch_right:
        fetch.start()
    fetch_left.start()
    fetch_weight.start()
    fetch_bias.start()

    turns = cols * period // LANES
    cycles = n // period

    def spread_half(h):
        fetch_right[h].wait()
        for s in range(local):
            for t in range(turns * cycles):
                rspread[t, s * TILE : (s + 1) * TILE] = right_ref[
                    s, h * TILE : (h + 1) * TILE, t * LANES : (t + 1) * LANES
                ].astype(jnp.float32)

    def pack_half(h, first, count):
        def pack(step, carry):
            chunk, cycle = step // count, first + lax.rem(step, count)
            tiles = [
                [
                    rspread[
                        cycle * turns + t,
                        pl.ds(chunk * period + e, local, stride=TILE),
                    ].astype(jnp.bfloat16)
                    for t in range(turns)
                ]
                for e in range(period)
            ]
            for d, outs in enumerate(pack_columns(cols, period, tiles)):
                for u, out in enumerate(outs):
                    sbuf[
                        h * per_half + chunk, cycle * period + d, :,
                        u * LANES : (u + 1) * LANES,
                    ] = out
            return carry

        lax.fori_loop(0, per_half * count, pack, 0)

    def send_right(group, to):
        first, count = groups[group]
        pltpu.make_async_remote_copy(
            src_ref=sbuf.at[pl.ds(first, count), to],
            dst_ref=rbuf.at[pl.ds(first, count), me],
            send_sem=rsend,
            recv_sem=rrecv.at[group, layer],
            device_id={"col": to},
            device_id_type=MESH,
        ).start()

    def send_layer(group, target, own=False):
        for p in range(int(own), span):
            send_right(group, target * span + lax.rem(place_in + p, span))

    def arrival(group, source, number):
        first, count = groups[group]
        slots = pl.ds(source * span, number)
        return pltpu.make_async_remote_copy(
            src_ref=sbuf.at[pl.ds(first, count), slots],
            dst_ref=rbuf.at[pl.ds(first, count), slots],
            send_sem=rsend,
            recv_sem=rrecv.at[group, source],
            device_id={"col": mirror},
            device_id_type=MESH,
        )

    def lcopy(slot, to):
        return pltpu.make_async_remote_copy(
            src_ref=lbuf.at[slot],
            dst_ref=lbuf.at[slot],
            send_sem=lsend,
            recv_sem=lrecv.at[slot],
            device_id={"col": to},
            device_id_type=MESH,
        )

    mates_near = [
        sibling * span + lax.rem(place_in + 2 * j, span) for j in range(span // 2)
    ]
    mates_own = [
        layer * span + lax.rem(place_in + 2 * j, span) for j in range(1, span // 2)
    ]
    mates = mates_near + mates_own

    half_cycles = cycles // 2
    mine = jnp.where(low, 0, half_cycles)
    theirs = half_cycles - mine
    early = jnp.where(is_inner, theirs, mine)
    spread_half(0)
    pack_half(0, early, half_cycles)
    pl.semaphore_wait(barrier, span)

    @pl.when(is_inner)
    def _():
        greet(layer_in, mirror)
        send_layer(0, inner)

    @pl.when(jnp.logical_not(is_inner))
    def _():
        for p in range(span):
            greet(edges_in, sibling * span + p)
        send_layer(0, sibling)

    pack_half(0, half_cycles - early, half_cycles)
    fetch_left.wait()
    for s in range(local):
        lspread[s * rows : (s + 1) * rows, :width] = left_ref[s].astype(jnp.float32)
    lane = lane_index()
    join = LANES // width
    for t in range(rows // join):
        block = lspread[pl.ds(t * join, local, stride=rows), :]
        for k in range(1, join):
            piece = lspread[pl.ds(t * join + k, local, stride=rows), :]
            block = pick(lane, k * width, block, turn_lanes(piece, k * width))
        lbuf[me, :, t * LANES : (t + 1) * LANES] = block.astype(jnp.bfloat16)

    @pl.when(is_inner)
    def _():
        pl.semaphore_wait(edges_in, span)
        pl.semaphore_wait(layer_in, 1)
        greet(far_in, mirror)
        for to in [mirror] + mates + [partner]:
            lcopy(me, to).start()
        send_layer(0, layer, own=True)
        send_layer(0, sibling)
        pl.semaphore_wait(far_in, 1)
        greet(all_in, near)
        send_layer(0, outer)

    @pl.when(jnp.logical_not(is_inner))
    def _():
        pl.semaphore_wait(all_in, 1)
        for to in [mirror] + mates + [partner]:
            lcopy(me, to).start()
        send_layer(0, layer, own=True)
        send_layer(0, inner)
        send_layer(0, outer)

    for h in range(1, halves):
        spread_half(h)
        pack_half(h, 0, cycles)
    own = pltpu.make_async_copy(sbuf.at[:, me], rbuf.at[:, me], loads.at[0])
    own.start()

    lcopy(mirror, me).wait_recv()
    for to in mates + [partner]:
        lcopy(mirror, to).start()

    later = range(1, rest)

    @pl.when(is_inner & low)
    def _():
        for group in later:
            send_layer(group, inner)
            send_layer(group, sibling)
            send_layer(group, layer, own=True)
            send_layer(group, outer)

    def send_part(group, target, part):
        for p in range(span // 2):
            turn = lax.rem(place_in + p, span // 2)
            send_right(group, target * span + part * (span // 2) + turn)

    @pl.when(is_inner & jnp.logical_not(low))
    def _():
        for group in later:
            send_layer(group, sibling)
            send_layer(group, layer, own=True)
        for group in later[:-1]:
            send_layer(group, outer)
        for group in later[:-1]:
            send_part(group, inner, 0)
        send_part(later[-1], outer, 0)
        for group in later[:-1]:
            send_part(group, inner, 1)
        for p in range(1, span // 2):
            send_right(later[-1], inner * span + p)
        send_part(later[-1], outer, 1)
        send_right(later[-1], inner * span)
        send_part(later[-1], inner, 1)

    @pl.when(jnp.logical_not(is_inner))
    def _():
        for group in later:
            send_layer(group, sibling)
            send_layer(group, layer, own=True)
        send_layer(rest, outer)
        send_layer(rest, inner)

    fetch_weight.wait()
    fetch_bias.wait()
    for start in range(0, channels, LANES):
        chosen = swap_matrix(width, width, start, LANES, channels)
        block = jnp.dot(chosen, weight_ref[...], preferred_element_type=jnp.float32)
        wturn[:, start : start + LANES] = block.T.astype(jnp.bfloat16)
    last[...] = wturn[:, channels - deep :]
    pair = bias_ref.shape[1]
    turned = jnp.broadcast_to(bias_ref[...] * float(seqs), (LANES, pair)).T
    bias_turned[:, :LANES] = turned
    bias_turned[:, LANES:] = turned

    for source in mates:
        for slot in (source, other(source)):
            lcopy(slot, me).wait_recv()
            lcopy(slot, partner).start()
    for source in [me] + mates:
        source = source + 1 - 2 * lax.rem(source, 2)
        for slot in (source, other(source)):
            lcopy(slot, me).wait_recv()
    for s in range(0, n, LANES // TILE):
        block = jnp.concatenate([lbuf[s + p] for p in range(LANES // TILE)], axis=0)
        lturn[:, s * TILE : s * TILE + LANES] = block.T

    def place(chunk, source):
        for p in range(span):
            slot = source * span + p
            start = pl.multiple_of(slot * TILE, TILE)
            block = [rbuf[chunk, slot, :, u * LANES : (u + 1) * LANES] for u in range(turns)]
            for e, wide in enumerate(unpack_columns(cols, period, block)):
                rwide[pl.ds(start, TILE), e * LANES : (e + 1) * LANES] = wide

    def multiply(step):
        lanes = slice(step * 2 * LANES, (step + 1) * 2 * LANES)
        product = jnp.dot(
            lturn[...], rwide[:, lanes], preferred_element_type=jnp.float32
        ).astype(jnp.bfloat16)
        for side_e in range(2):
            at = (step * 2 + side_e) * width
            for i in range(rows):
                side = (i % 2) * LANES
                flat[i // 2, at : at + width, side : side + LANES] = product[
                    i * width : (i + 1) * width, side_e * LANES : (side_e + 1) * LANES
                ]

    def project(chunk, step):
        update = jnp.dot(
            wturn[:, chunk * deep : (chunk + 1) * deep], flat[step],
            preferred_element_type=jnp.float32,
        )
        partial[step] = update + (partial[step] if chunk else bias_turned[...])

    own.wait()
    for group, (first, count) in enumerate(groups[:rest]):
        arrival(group, layer, span - 1).wait_recv()
        place(first, layer)
        arrival(group, sibling, span).wait_recv()
        place(first, sibling)
        if group < 2:
            arrival(rest if group else group, outer, span).wait_recv()
        place(first, outer)
        arrival(group, inner, span).wait_recv()
        place(first, inner)
        for chunk in range(first, first + count):
            if chunk > first:
                for source in range(LAYERS):
                    place(chunk, source)
            for step in range(period // 2):
                multiply(step)
            if chunk < chunks - 1:
                for step in range(rows // 2):
                    project(chunk, step)

    pltpu.make_async_remote_copy(
        src_ref=sbuf.at[:, pl.ds(0, n - 1)],
        dst_ref=rbuf.at[:, pl.ds(0, n - 1)],
        send_sem=rsend,
        recv_sem=rrecv.at[0, 0],
        device_id={"col": mirror},
        device_id_type=MESH,
    ).wait_send()
    pltpu.make_async_remote_copy(
        src_ref=lbuf.at[pl.ds(0, n - 1)],
        dst_ref=lbuf.at[pl.ds(0, n - 1)],
        send_sem=lsend,
        recv_sem=lrecv.at[0],
        device_id={"col": mirror},
        device_id_type=MESH,
    ).wait_send()


def finish_kernel(seqs, cols, flat, partial, last, out_hbm, out_ref, sems):
    steps = flat.shape[0]
    per = steps // STORES
    copies = []
    for store in range(STORES):
        for step in range(store * per, (store + 1) * per):
            update = jnp.dot(last[...], flat[step], preferred_element_type=jnp.float32)
            update = ((update + partial[step]) * (1.0 / seqs)).astype(out_ref.dtype)
            for side in range(2):
                block = update[:, side * LANES : (side + 1) * LANES].T
                out_ref[2 * step + side] = block[:cols]
        at = pl.ds(2 * store * per, 2 * per)
        copies.append(pltpu.make_async_copy(out_ref.at[at], out_hbm.at[at], sems.at[store]))
        copies[-1].start()
    for copy in copies:
        copy.wait()


def packed_call(n, left, right, out_weight, out_bias):
    local, rows, width = left.shape
    cols = right.shape[1] // n
    pair = out_weight.shape[1]
    seqs = local * n
    period = LANES // math.gcd(cols, LANES)
    chunks = width // period
    lanes = cols * period
    hbm = pl.BlockSpec(memory_space=pltpu.HBM)
    vmem = pl.BlockSpec(memory_space=pltpu.VMEM)
    dma, regular = pltpu.SemaphoreType.DMA, pltpu.SemaphoreType.REGULAR
    bf16, f32 = jnp.bfloat16, jnp.float32
    parts = pl.pallas_call(
        functools.partial(packed_kernel, n, cols, period),
        out_shape=(
            jax.ShapeDtypeStruct((rows // 2, period * width, 2 * LANES), bf16),
            jax.ShapeDtypeStruct((rows // 2, pair, 2 * LANES), f32),
            jax.ShapeDtypeStruct((pair, period * width), bf16),
        ),
        in_specs=[hbm] * 4,
        out_specs=(vmem,) * 3,
        scratch_shapes=[
            pltpu.VMEM((local, rows, width), bf16),
            pltpu.VMEM((local, width, n * cols), bf16),
            pltpu.VMEM((width * width, pair), bf16),
            pltpu.VMEM((1, pair), f32),
            pltpu.VMEM((pair, 2 * LANES), f32),
            pltpu.VMEM((local * rows, LANES), f32),
            pltpu.VMEM((n * cols // LANES, local * TILE, LANES), f32),
            pltpu.VMEM((chunks, n, local, lanes), bf16),
            pltpu.VMEM((chunks, n, local, lanes), bf16),
            pltpu.VMEM((n, local, rows * width), bf16),
            pltpu.VMEM((seqs, period * LANES), bf16),
            pltpu.VMEM((rows * width, seqs), bf16),
            pltpu.VMEM((pair, width * width), bf16),
            dma(()), dma((2 + chunks - chunks * TILE // width, LAYERS)), dma(()), dma((n,)),
            dma((3 + width // TILE,)), regular, regular, regular, regular,
        ],
        compiler_params=pltpu.CompilerParams(
            collective_id=0, has_side_effects=True, vmem_limit_bytes=40 * 1024 * 1024
        ),
    )(*(pltpu.with_memory_space_constraint(x, pltpu.HBM) for x in (left, jnp.transpose(right, (0, 2, 1)), out_weight, out_bias.reshape(1, pair))))
    return pl.pallas_call(
        functools.partial(finish_kernel, seqs, cols),
        out_shape=jax.ShapeDtypeStruct((rows, cols, pair), bf16),
        in_specs=[vmem] * 3,
        out_specs=hbm,
        scratch_shapes=[pltpu.VMEM((rows, cols, pair), bf16), dma((STORES,))],
        compiler_params=pltpu.CompilerParams(vmem_limit_bytes=16 * 1024 * 1024),
    )(*(pltpu.with_memory_space_constraint(x, pltpu.VMEM) for x in parts))


def packs(n, left, right):
    local, rows, width = left.shape
    cols = right.shape[1] // n
    period = LANES // math.gcd(cols, LANES)
    return (
        local == TILE and cols <= LANES and rows % (2 * STORES) == 0 and rows <= 32
        and LANES % width == 0 and rows % (LANES // width) == 0
        and width % TILE == 0 and TILE % period == 0 and period % 2 == 0
        and n % period == 0 and n % (LANES // TILE) == 0 and n % (2 * LAYERS) == 0
        and width // period % (width // TILE) == 0 and n // period % 2 == 0
    )


def flip(x_ref, o_ref, h):
    chunks, columns, lanes = o_ref.shape
    part = x_ref.shape[1] // chunks
    step = 2 * LANES
    for start in range(0, columns, step):
        piece = x_ref[:, h * part : (h + 1) * part, start : start + step]
        o_ref[h, start : start + step] = piece.reshape(lanes, step).T


def swap_matrix(first, minor, start, rows, columns):
    row = lax.broadcasted_iota(jnp.int32, (rows, columns), 0) + start
    column = lax.broadcasted_iota(jnp.int32, (rows, columns), 1)
    shift = first.bit_length() - 1
    wanted = (row & (first - 1)) * minor + (row >> shift)
    return jnp.where(column == wanted, 1.0, 0.0).astype(jnp.bfloat16)


def kernel(
    n, width, cols, rows, chunks, given_ref, left_ref, weight_ref, bias_ref, out_ref,
    right_ref, rbuf, lbuf, rwide, lturn, wturn, flat, partial,
    rsend, rrecv, lsend, lrecv, fsend, own,
):
    me = lax.axis_index("col")
    place = lax.rem(me, GROUP)
    mates = [me - place + lax.rem(place + j, GROUP) for j in range(1, GROUP)]
    hops = n // GROUP
    local = left_ref.shape[0]
    seqs = n * local
    part = width // chunks

    def rcopy(h, k):
        to = lax.rem(me + k, n)
        start = pl.multiple_of(to * cols, TILE)
        return pltpu.make_async_remote_copy(
            src_ref=right_ref.at[h, pl.ds(start, cols)],
            dst_ref=rbuf.at[h, me],
            send_sem=rsend.at[h, k],
            recv_sem=rrecv.at[h, me],
            device_id={"col": to},
            device_id_type=MESH,
        )

    def lcopy(src, slot, to, send):
        return pltpu.make_async_remote_copy(
            src_ref=src,
            dst_ref=lbuf.at[slot],
            send_sem=send,
            recv_sem=lrecv.at[slot],
            device_id={"col": to},
            device_id_type=MESH,
        )

    barrier = pltpu.get_barrier_semaphore()
    for k in range(1, n):
        pl.semaphore_signal(
            barrier, inc=1, device_id={"col": lax.rem(me + k, n)}, device_id_type=MESH
        )
    flip(given_ref, right_ref, 0)
    pl.semaphore_wait(barrier, n - 1)

    sends = []
    for k in range(1, hops):
        sends.append(lcopy(left_ref, me, lax.rem(me + GROUP * k, n), lsend.at[k]))
    for j, mate in enumerate(mates):
        sends.append(lcopy(left_ref, me, mate, fsend.at[0, j]))
    for k in range(1, n):
        sends.append(rcopy(0, k))
    for copy in sends:
        copy.start()
    for h in range(1, chunks):
        flip(given_ref, right_ref, h)
    mine_left = pltpu.make_async_copy(left_ref, lbuf.at[me], own.at[chunks])
    mine_left.start()

    rwide[...] = jnp.zeros_like(rwide)
    channels = width * width
    for start in range(0, channels, LANES):
        chosen = swap_matrix(width, width, start, LANES, channels)
        block = jnp.dot(chosen, weight_ref[...], preferred_element_type=jnp.float32)
        wturn[:, start : start + LANES] = block.T.astype(jnp.bfloat16)
    for h in range(1, chunks):
        later = [rcopy(h, k) for k in range(1, n)]
        for copy in later:
            copy.start()
        sends += later
    mine = []
    for h in range(chunks):
        block = right_ref.at[h, pl.ds(pl.multiple_of(me * cols, TILE), cols)]
        mine.append(pltpu.make_async_copy(block, rbuf.at[h, me], own.at[h]))
        mine[h].start()
    swap = swap_matrix(TILE, part, 0, TILE * part, TILE * part)

    forwards = []
    for k in range(1, hops):
        slot = lax.rem(me + n - GROUP * k, n)
        lcopy(left_ref, slot, mates[0], lsend.at[k]).wait_recv()
        for j, mate in enumerate(mates):
            forward = lcopy(lbuf.at[slot], slot, mate, fsend.at[k, j])
            forward.start()
            forwards.append(forward)
    for k in range(hops):
        for j, mate in enumerate(mates):
            slot = lax.rem(mate + n - GROUP * k, n)
            lcopy(left_ref, slot, mate, fsend.at[k, j]).wait_recv()
    mine_left.wait()
    per = TILE // local
    blocks = []
    for group in range(seqs // TILE):
        parts = [lbuf[group * per + p] for p in range(per)]
        if per > 1:
            parts = [piece.astype(jnp.float32) for piece in parts]
            blocks.append(jnp.concatenate(parts, axis=0).astype(jnp.bfloat16))
        else:
            blocks.append(parts[0])
    lturn[...] = jnp.concatenate(blocks, axis=0).T

    def turn(h, start, block):
        turned = lax.dot_general(
            swap, block, (((1,), (1,)), ((), ())), preferred_element_type=jnp.float32
        ).astype(jnp.bfloat16)
        for e in range(part):
            at = (h * part + e) * LANES
            rwide[pl.ds(start, TILE), at : at + cols] = turned[e * TILE : (e + 1) * TILE]

    def arrive(h):
        def one(k, carry):
            slot = lax.rem(me + n - k, n)
            pltpu.make_async_remote_copy(
                src_ref=right_ref.at[h, pl.ds(0, cols)],
                dst_ref=rbuf.at[h, slot],
                send_sem=rsend.at[h, k],
                recv_sem=rrecv.at[h, slot],
                device_id={"col": slot},
                device_id_type=MESH,
            ).wait_recv()
            if per == 1:
                turn(h, pl.multiple_of(slot * TILE, TILE), rbuf[h, slot])
            return carry

        mine[h].wait()
        if per == 1:
            turn(h, pl.multiple_of(me * TILE, TILE), rbuf[h, me])
        lax.fori_loop(1, n, one, 0)
        if per > 1:
            for group in range(seqs // TILE):
                parts = [rbuf[h, group * per + p] for p in range(per)]
                turn(h, group * TILE, jnp.concatenate(parts, axis=1))

    count = flat.shape[0] * 2

    def multiply(base, h):
        def outer(step, carry):
            lanes = pl.ds(pl.multiple_of(step * 2 * LANES, 2 * LANES), 2 * LANES)
            product = jnp.dot(
                lturn[base * width : (base + count) * width, :],
                rwide[:, lanes],
                preferred_element_type=jnp.float32,
            ).astype(jnp.bfloat16)
            for side_e in range(2):
                at = pl.ds(pl.multiple_of((step * 2 + side_e) * width, width), width)
                for i in range(count):
                    side = (i % 2) * LANES
                    flat[i // 2, at, side : side + LANES] = product[
                        i * width : (i + 1) * width, side_e * LANES : (side_e + 1) * LANES
                    ]
            return carry

        lax.fori_loop(h * part // 2, (h + 1) * part // 2, outer, 0)

    deep = part * width
    early = rows == count and chunks > 1

    def project_early(step, carry):
        partial[step] = jnp.dot(
            wturn[:, : channels - deep],
            flat[step, : channels - deep],
            preferred_element_type=jnp.float32,
        )
        return carry

    for h in range(chunks):
        arrive(h)
        if rows == count:
            multiply(0, h)
        if early and h == chunks - 2:
            lax.fori_loop(0, count // 2, project_early, 0)

    skip = channels - deep if early else 0
    for base in range(0, rows, count):
        if rows != count:
            for h in range(chunks):
                multiply(base, h)

        def project(step, carry):
            update = jnp.dot(
                wturn[:, skip:], flat[step, skip:], preferred_element_type=jnp.float32
            )
            if early:
                update = update + partial[step]
            update = update.T * (1.0 / seqs) + bias_ref[...]
            update = update.astype(out_ref.dtype)
            out_ref[base + 2 * step] = update[:cols]
            out_ref[base + 2 * step + 1] = update[LANES : LANES + cols]
            return carry

        lax.fori_loop(0, count // 2, project, 0)

    for copy in sends + forwards:
        copy.wait_send()


def on_device(n, left, right, out_weight, out_bias):
    if packs(n, left, right):
        return packed_call(n, left, right, out_weight, out_bias)
    local, rows, width = left.shape
    cols = right.shape[1] // n
    pair = out_weight.shape[1]
    seqs = local * n
    chunks = 2 if local * width % (4 * LANES) == 0 else 1
    rows_step = min(rows, 32)
    vmem = pl.BlockSpec(memory_space=pltpu.VMEM)
    dma = pltpu.SemaphoreType.DMA
    return pl.pallas_call(
        functools.partial(kernel, n, width, cols, rows, chunks),
        out_shape=jax.ShapeDtypeStruct((rows, cols, pair), jnp.bfloat16),
        in_specs=[vmem] * 4,
        out_specs=vmem,
        scratch_shapes=[
            pltpu.VMEM((chunks, right.shape[1], local * width // chunks), jnp.bfloat16),
            pltpu.VMEM((chunks, n, cols, local * width // chunks), jnp.bfloat16),
            pltpu.VMEM((n, local, rows * width), jnp.bfloat16),
            pltpu.VMEM((seqs, width * LANES), jnp.bfloat16),
            pltpu.VMEM((rows * width, seqs), jnp.bfloat16),
            pltpu.VMEM((pair, width * width), jnp.bfloat16),
            pltpu.VMEM((rows_step // 2, width * width, 2 * LANES), jnp.bfloat16),
            pltpu.VMEM((rows_step // 2, pair, 2 * LANES), jnp.float32),
            dma((chunks, n)), dma((chunks, n)),
            dma((n // GROUP,)), dma((n,)), dma((n // GROUP, GROUP)), dma((chunks + 1,)),
        ],
        compiler_params=pltpu.CompilerParams(
            collective_id=0, has_side_effects=True, vmem_limit_bytes=40 * 1024 * 1024
        ),
    )(jnp.transpose(right, (0, 2, 1)), left.reshape(local, rows * width), out_weight, out_bias.reshape(1, pair))


def solution(mesh):
    return jax.shard_map(
        functools.partial(on_device, mesh.shape["col"]),
        mesh=mesh,
        in_specs=(P("col", "groups", None), P("col", "groups", None), P(), P()),
        out_specs=P("groups", "col", None),
        check_vma=False,
    )
```
